32 devices in a mesh: owner: 4 (over x, core), rows: 8 (over z, y).
Axes of the slice: x: 2, y: 2, z: 4, core: 2. Of those that a mesh axis runs over, the one named last changes fastest.
Arguments:
- master_gate: float32 [64, 2048, 1408], P('owner', 'rows'), may hold values from -0.1875 to 0.1875
- master_up: float32 [64, 2048, 1408], P('owner', 'rows'), may hold values from -0.1875 to 0.1875
- router_weight: float32 [2048, 64], P('rows', 'owner'), may hold values from -0.125 to 0.125
- router_gain: float32 [2048], P('rows'), may hold values from 0.25 to 1.75
Outputs:
- final_gate: bfloat16 [64, 2048, 1408], P('owner', None, 'rows')
- final_up: bfloat16 [64, 2048, 1408], P('owner', None, 'rows')
- scale_gate: float32 [64, 1408], P('owner', 'rows')
- scale_up: float32 [64, 1408], P('owner', 'rows')
- serve_router: bfloat16 [2048, 64], replicated
The draws below stay inside these ranges and needn't reach their ends.
All inputs are finite; a program needn't handle non-finite values. Where the reference program divides by a largest or mean magnitude, that divisor is 1e-20 or more.
Results may differ from the reference program's by a relative error of at most 0.001.
Values may be sent and summed in bfloat16 or wider, within the bound.
A program may use at most 192 MiB of HBM per device.

```python
import jax
import jax.numpy as jnp

EXPERTS = 64
D_MODEL = 2048
D_EXPERT = 1408


def strengthened(entries, key, source, target, blocks, factor):
    owner, partner = [(jnp.arange(entries.shape[dim]) // (entries.shape[dim] // blocks)).reshape([-1 if axis == dim else 1 for axis in range(entries.ndim)]) for dim in (source, target)]
    chosen = jax.random.permutation(key, blocks)[partner]
    strong = (owner == chosen) | (owner == (partner + blocks // 2) % blocks)
    return jnp.where(strong, factor * entries, entries)


def levels(stream_key, dims, pieces, low, largest):
    level = 1.0
    for position, shards_of in pieces:
        steps = jax.random.uniform(jax.random.fold_in(jax.random.fold_in(stream_key, 6), position), (shards_of,), jnp.float32, low / len(pieces), largest / len(pieces))
        level = level * jnp.repeat(jnp.exp(steps), dims[position] // shards_of).reshape((-1,) + (1,) * (len(dims) - 1 - position))
    return level


def centred(rng, extent, spread, limit, shards=(), dtype=jnp.bfloat16):
    result = spread * jax.random.normal(rng, extent, jnp.float32)
    if shards:
        result = result * levels(rng, extent, shards, -0.22, 0.18)
    return jnp.clip(result, -limit, limit).astype(dtype)


def gaussian_with(own_key, shape, scale, bound, cuts, heavy, dtype=jnp.bfloat16):
    drawn = scale * jax.random.normal(own_key, shape, jnp.float32)
    if cuts:
        drawn = drawn * levels(own_key, shape, cuts, -0.22, 0.18)
    return jnp.clip(strengthened(drawn, jax.random.fold_in(own_key, 3), *heavy), -bound, bound).astype(dtype)


def setup_inputs(seed: int = 0) -> dict:
    streams_of = jax.random.split(jax.random.key(seed), 5)
    return {
        "master_gate": gaussian_with(streams_of[0], (EXPERTS, D_MODEL, D_EXPERT), D_MODEL ** -0.5, 0.1875, ((0, 4), (1, 8)), (1, 2, 8, 2.0), jnp.float32),
        "master_up": gaussian_with(streams_of[1], (EXPERTS, D_MODEL, D_EXPERT), D_MODEL ** -0.5, 0.1875, ((0, 4), (1, 8)), (1, 2, 8, 2.0), jnp.float32),
        "router_weight": centred(streams_of[2], (D_MODEL, EXPERTS), D_MODEL ** -0.5, 0.125, ((0, 8), (1, 4)), jnp.float32),
        "router_gain": jnp.clip(1.0 + 0.15 * jax.random.normal(streams_of[3], (D_MODEL,), jnp.float32), 0.25, 1.75),
    }


def reference(master_gate, master_up, router_weight, router_gain):
    scale_gate = jnp.max(jnp.abs(master_gate), axis=1)
    final_gate = (master_gate / jnp.expand_dims(scale_gate, 1)).astype(jnp.bfloat16)
    scale_up = jnp.max(jnp.abs(master_up), axis=1)
    final_up = (master_up / jnp.expand_dims(scale_up, 1)).astype(jnp.bfloat16)
    serve_router = (router_weight * router_gain[:, None]).astype(jnp.bfloat16)
    return final_gate, final_up, scale_gate, scale_up, serve_router
```

```python
import functools

import jax
import jax.numpy as jnp
from jax import lax
from jax.experimental import pallas as pl
from jax.experimental.pallas import tpu as pltpu
from jax.sharding import PartitionSpec as P

MESH = pl.DeviceIdType.MESH
LANES = 128
SUBLANES = 8
PACKED = 16
SLOTS = 5
DIRECT = 3
LANDINGS = 4
VMEM_FOR_BLOCKS = 48 * 1024 * 1024
VMEM_FOR_REST = 2 * 1024 * 1024


def kernel(
    owners,
    peers,
    gate,
    up,
    router_hbm,
    gain_hbm,
    out_gate,
    out_up,
    out_router,
    out_scale_gate,
    out_scale_up,
    slots,
    seen,
    opening,
    largest_first,
    largest_rest,
    scales_first,
    scales_rest,
    parts_first,
    parts_rest,
    partial_first,
    partial_rest,
    across_first,
    across_rest,
    send,
    router,
    gain,
    row,
    slot_sem,
    small_sem,
    send_sem,
    recv_sem,
    seen_send,
    seen_recv,
    part_send,
    part_recv,
    across_send,
    across_recv,
    whole_send,
    whole_recv,
    router_send,
    router_recv,
):
    owner, me = lax.axis_index("owner"), lax.axis_index("rows")
    experts, rows, width = gate.shape
    tiles = width // LANES
    cut = width // peers
    near = peers // 2
    spot = lax.rem(me, near)
    masters, outs = (gate, up), (out_gate, out_up)
    largest, parts = (largest_first, largest_rest), (parts_first, parts_rest)
    partial, across = (partial_first, partial_rest), (across_first, across_rest)
    scales = (scales_first, scales_rest)
    lanes = pl.ds(pl.multiple_of(me * rows, LANES), rows)

    def partner(k):
        bits = [1 << b for b in range(peers.bit_length() - 1) if k >> b & 1]
        return sum((bit - 2 * bit * lax.rem(me // bit, 2) for bit in bits), me)

    def remote(src, dst, sent, received, to):
        return pltpu.make_async_remote_copy(
            src_ref=src,
            dst_ref=dst,
            send_sem=sent,
            recv_sem=received,
            device_id=to,
            device_id_type=MESH,
        )

    stream = [(0, 0, SUBLANES), (0, 0, DIRECT - 1)]
    if experts > SUBLANES:
        stream.append((0, SUBLANES, experts - SUBLANES))
    stream += [(1, 0, experts), (0, DIRECT - 1, experts - DIRECT + 1), (1, 0, experts)]
    bases = [sum(length for _, _, length in stream[:q]) for q in range(len(stream))]
    total = sum(length for _, _, length in stream)

    def fetch(m, e, i):
        s = lax.rem(i, SLOTS)
        return pltpu.make_async_copy(masters[m].at[e], slots.at[s], slot_sem.at[s])

    def fetch_start(i):
        for (m, first, length), base in zip(stream, bases):
            if isinstance(i, int):
                if base <= i < base + length:
                    fetch(m, first + i - base, i).start()
            else:

                @pl.when(jnp.logical_and(i >= base, i < base + length))
                def _():
                    fetch(m, first + i - base, i).start()

    def arrived(q, i):
        m, first, _ = stream[q]
        fetch(m, first + i, bases[q] + i).wait()
        return first + i, lax.rem(bases[q] + i, SLOTS)

    def following(q, i, steps):
        ahead = bases[q] + i + SLOTS
        low = bases[q] + SLOTS
        for (m, first, length), base in zip(stream, bases):
            if base + length <= low or base >= low + steps:
                continue
            if base <= low and base + length >= low + steps:
                fetch(m, first + ahead - base, ahead).start()
            else:

                @pl.when(jnp.logical_and(ahead >= base, ahead < base + length))
                def _():
                    fetch(m, first + ahead - base, ahead).start()

    def spots(m, e, c, first):
        k = m * experts + e - (0 if first else SUBLANES)
        return (k // SUBLANES) * tiles + c, pl.ds(k % SUBLANES if isinstance(k, int) else lax.rem(k, SUBLANES), 1)

    def measure(m, e, s, first):
        found = []
        for c in range(tiles):
            x = slots[s, :, c * LANES : (c + 1) * LANES]
            tile, sub = spots(m, e, c, first)
            found.append(jnp.max(jnp.abs(x), axis=0, keepdims=True))
            largest[0 if first else 1][tile, sub, :] = found[-1]
        return found

    def maxima(q, start, first):
        m, _, length = stream[q]

        def body(i, _):
            e, s = arrived(q, i)
            measure(m, e, s, first)
            following(q, i, length)
            return 0

        lax.fori_loop(start, length, body, 0)

    def seen_copy(e, k):
        return remote(
            seen.at[e, 0, pl.ds(0, tiles)],
            seen.at[e, k, pl.ds(0, tiles)],
            seen_send.at[e, k],
            seen_recv.at[e, k],
            {"rows": partner(k)},
        )

    def part_copy(stage, k):
        per = parts[stage].shape[1]
        to = partner(k)
        return remote(
            largest[stage].at[pl.ds(lax.rem(to, near) * per, per)],
            parts[stage].at[k],
            part_send.at[stage, k],
            part_recv.at[stage, k],
            {"rows": to},
        )

    def across_copy(stage):
        return remote(
            partial[stage],
            across[stage],
            across_send.at[stage],
            across_recv.at[stage],
            {"rows": partner(near)},
        )

    def share(stage, of):
        per = parts[stage].shape[1]
        return scales[stage].at[pl.ds(of * per, per)]

    def whole_copy(stage, k):
        return remote(
            share(stage, spot),
            share(stage, spot),
            whole_send.at[stage, k],
            whole_recv.at[stage, k],
            {"rows": partner(k)},
        )

    def scatter(stage):
        for k in range(1, near):
            part_copy(stage, k).start()

    def reduce(stage):
        per = parts[stage].shape[1]
        most = largest[stage][pl.ds(spot * per, per)]
        for k in range(1, near):
            part_copy(stage, k).wait_recv()
            most = jnp.maximum(most, parts[stage][k])
        partial[stage][...] = most
        across_copy(stage).start()

    def spread(stage):
        across_copy(stage).wait_recv()
        share(stage, spot)[...] = jnp.maximum(partial[stage][...], across[stage][...])
        for k in range(1, near):
            whole_copy(stage, k).start()

    def gathered(stage):
        across_copy(stage).wait_send()
        for k in range(1, near):
            part_copy(stage, k).wait_send()
            there = share(stage, lax.rem(partner(k), near))
            pltpu.make_async_copy(there, there, whole_recv.at[stage, k]).wait()
            whole_copy(stage, k).wait_send()

    def send_copy(m, k, e, length):
        to = partner(k)
        return remote(
            send.at[m, pl.ds(e, length), pl.ds(pl.multiple_of(to * cut, PACKED), cut), :],
            outs[m].at[pl.ds(e, length), :, lanes],
            send_sem.at[m, k],
            recv_sem.at[m, k],
            {"rows": to},
        )

    def keep_copy(m, e, length):
        return pltpu.make_async_copy(
            send.at[m, pl.ds(e, length), pl.ds(pl.multiple_of(me * cut, PACKED), cut), :],
            outs[m].at[pl.ds(e, length), :, lanes],
            send_sem.at[m, 0],
        )

    def one(m, e, s, scale_of):
        for c in range(tiles):
            x = slots[s, :, c * LANES : (c + 1) * LANES]
            send[m, e, c * LANES : (c + 1) * LANES, :] = (x / scale_of(c)).T.astype(send.dtype)
        for k in range(1, peers):
            send_copy(m, k, e, 1).start()
        keep_copy(m, e, 1).start()

    def bulk(q, start, stop, first):
        m, _, _ = stream[q]

        def body(i, _):
            e, s = arrived(q, i)

            def scale_of(c):
                tile, sub = spots(m, e, c, first)
                return scales[0 if first else 1][tile, sub, :]

            one(m, e, s, scale_of)
            following(q, i, stream[q][2])
            return 0

        lax.fori_loop(start, stop, body, 0)

    def early(q, i):
        e = stream[q][1] + i
        for k in range(1, peers):
            seen_copy(e, k).wait_recv()
        opening[e, :tiles, :] = jnp.max(seen[e, :, :tiles, :], axis=0)
        _, s = arrived(q, i)
        one(0, e, s, lambda c: opening[e, c : c + 1, :])
        fetch_start(bases[q] + i + SLOTS)

    depth = router.shape[0]
    mine = pl.ds(pl.multiple_of(owner * depth, PACKED), depth)

    def block(of):
        return out_router.at[mine, pl.ds(pl.multiple_of(of * rows, LANES), rows)]

    def router_across():
        return remote(row, block(me), router_send.at[0], router_recv.at[0], {"rows": partner(near)})

    def router_near(k, far):
        of = partner(near) if far else me
        return remote(
            block(of) if far else row,
            block(of),
            router_send.at[1 + 2 * k + far],
            router_recv.at[1 + 2 * k + far],
            {"rows": partner(k)},
        )

    def router_near_arrival(k, far):
        there = block(partner(near + k) if far else partner(k))
        return pltpu.make_async_copy(there, there, router_recv.at[1 + 2 * k + far])

    def router_owner(j):
        return remote(
            out_router.at[mine],
            out_router.at[mine],
            router_send.at[peers + j],
            router_recv.at[peers + j],
            {"owner": lax.rem(owner + j, owners)},
        )

    def router_owner_arrival(j):
        from_owner = lax.rem(owner + owners - j, owners)
        there = out_router.at[pl.ds(pl.multiple_of(from_owner * depth, PACKED), depth)]
        return pltpu.make_async_copy(there, there, router_recv.at[peers + j])

    barrier = pltpu.get_barrier_semaphore()

    fetch_start(0)
    for k in range(1, peers):
        pl.semaphore_signal(barrier, inc=1, device_id={"rows": partner(k)}, device_id_type=MESH)
    for j in range(1, owners):
        pl.semaphore_signal(
            barrier,
            inc=1,
            device_id={"owner": lax.rem(owner + j, owners)},
            device_id_type=MESH,
        )
    for i in range(1, SLOTS):
        fetch_start(i)
    smalls = [
        pltpu.make_async_copy(router_hbm, router, small_sem.at[0]),
        pltpu.make_async_copy(gain_hbm, gain, small_sem.at[1]),
    ]
    for copy in smalls:
        copy.start()
    largest_first[...] = jnp.zeros_like(largest_first)
    largest_rest[...] = jnp.zeros_like(largest_rest)
    for e in range(DIRECT):
        _, s = arrived(0, e)
        found = measure(0, e, s, True)
        for c in range(tiles):
            seen[e, 0, c : c + 1, :] = found[c]
        if e == 0:
            pl.semaphore_wait(barrier, peers - 1 + owners - 1)
        for k in range(1, peers):
            seen_copy(e, k).start()
        fetch_start(e + SLOTS)
    for copy in smalls:
        copy.wait()
    row[...] = (router[...] * gain[...]).astype(row.dtype)
    router_across().start()
    keep_router = pltpu.make_async_copy(row, block(me), small_sem.at[0])
    keep_router.start()
    maxima(0, DIRECT, True)
    scatter(0)
    early(1, 0)
    reduce(0)
    early(1, 1)
    rest = 2
    if experts > SUBLANES:
        maxima(rest, 0, False)
        rest += 1
    maxima(rest, 0, False)
    rest += 1
    router_across().wait_recv()
    for k in range(1, near):
        router_near(k, 0).start()
        router_near(k, 1).start()
    spread(0)
    scatter(1)
    early(rest, 0)
    gathered(0)
    bulk(rest, 1, 2, True)
    reduce(1)
    bulk(rest, 2, 3, True)
    spread(1)
    bulk(rest, 3, SUBLANES - DIRECT + 1, True)
    gathered(1)
    if experts > SUBLANES:
        bulk(rest, SUBLANES - DIRECT + 1, experts - DIRECT + 1, False)
    keep_router.wait()
    router_across().wait_send()
    for k in range(1, near):
        for far in range(2):
            router_near_arrival(k, far).wait()
            router_near(k, far).wait_send()
    for j in range(1, owners):
        router_owner(j).start()
    bulk(rest + 1, 0, experts, False)

    for at in range(peers):

        @pl.when(me == at)
        def _():
            low = at * cut // LANES
            high = -(-(at + 1) * cut // LANES)
            for m in range(2):
                for e in range(0, experts, SUBLANES):
                    first = m == 0 and e == 0
                    found = []
                    for c in range(low, high):
                        k = m * experts + e - (0 if first else SUBLANES)
                        found.append(scales[0 if first else 1][(k // SUBLANES) * tiles + c])
                    found = jnp.concatenate(found, axis=1)
                    begin = at * cut - low * LANES
                    out = (out_scale_gate, out_scale_up)[m]
                    out[e : e + SUBLANES, :] = found[:, begin : begin + cut]

    for e in range(DIRECT):
        for k in range(1, peers):
            seen_copy(e, k).wait_send()
    for j in range(1, owners):
        router_owner_arrival(j).wait()
        router_owner(j).wait_send()
    for m in range(2):
        keep_copy(m, 0, experts).wait()
        for k in range(1, peers):
            send_copy(m, k, 0, experts).wait()


def land(*refs):
    arrays = len(refs) // 2
    ins, outs, sem = refs[:arrays], refs[arrays:-1], refs[-1]
    for i, (a, b) in enumerate(zip(ins, outs)):
        pieces = LANDINGS if a.shape[0] % LANDINGS == 0 and len(a.shape) == 3 else 1
        per = a.shape[0] // pieces
        for j in range(pieces):
            at = pl.ds(j * per, per)
            pltpu.make_async_copy(a.at[at], b.at[at], sem.at[i]).start()
    for i, (a, b) in enumerate(zip(ins, outs)):
        pltpu.make_async_copy(a, b, sem.at[i]).wait()


def fused(owners, peers, master_gate, master_up, router_weight, router_gain):
    experts, rows, width = master_gate.shape
    cut = width // peers
    near = peers // 2
    tiles = width // LANES
    padded = -(-tiles // SUBLANES) * SUBLANES
    groups = 2 * experts // SUBLANES
    first, rest = -(-tiles // near), -(-(groups - 1) * tiles // near)
    depth = router_weight.shape[1]
    anywhere = pl.BlockSpec(memory_space=pl.ANY)
    vmem = pl.BlockSpec(memory_space=pltpu.VMEM)
    hbm = pl.BlockSpec(memory_space=pltpu.HBM)
    dma = pltpu.SemaphoreType.DMA
    turned = jax.ShapeDtypeStruct((experts, cut, rows * peers), jnp.bfloat16)
    scale = jax.ShapeDtypeStruct((experts, cut), jnp.float32)

    def maxima(*shape):
        return pltpu.VMEM((*shape, SUBLANES, LANES), jnp.float32)

    landed = pl.pallas_call(
        functools.partial(kernel, owners, peers),
        out_shape=(
            turned,
            turned,
            jax.ShapeDtypeStruct((depth * owners, rows * peers), jnp.bfloat16),
            scale,
            scale,
        ),
        in_specs=[anywhere, anywhere, hbm, hbm],
        out_specs=(anywhere, anywhere, anywhere, vmem, vmem),
        scratch_shapes=[
            pltpu.VMEM((SLOTS, rows, width), jnp.float32),
            pltpu.VMEM((DIRECT, peers, padded, LANES), jnp.float32),
            pltpu.VMEM((DIRECT, padded, LANES), jnp.float32),
            maxima(first * near),
            maxima(rest * near),
            maxima(first * near),
            maxima(rest * near),
            maxima(near, first),
            maxima(near, rest),
            maxima(first),
            maxima(rest),
            maxima(first),
            maxima(rest),
            pltpu.VMEM((2, experts, width, rows), jnp.bfloat16),
            pltpu.VMEM((depth, rows), jnp.float32),
            pltpu.VMEM((1, rows), jnp.float32),
            pltpu.VMEM((depth, rows), jnp.bfloat16),
            dma((SLOTS,)),
            dma((2,)),
            dma((2, peers)),
            dma((2, peers)),
            dma((DIRECT, peers)),
            dma((DIRECT, peers)),
            dma((2, near)),
            dma((2, near)),
            dma((2,)),
            dma((2,)),
            dma((2, near)),
            dma((2, near)),
            dma((peers + owners,)),
            dma((peers + owners,)),
        ],
        compiler_params=pltpu.CompilerParams(
            collective_id=0,
            has_side_effects=True,
            vmem_limit_bytes=(4 * experts + 4 * SLOTS) * rows * width + VMEM_FOR_REST,
        ),
    )(master_gate, master_up, *(pltpu.with_memory_space_constraint(a, pltpu.HBM) for a in (router_weight.T, router_gain[None, :])))
    gate, up, router, scale_gate, scale_up = pl.pallas_call(
        land,
        out_shape=[jax.ShapeDtypeStruct(a.shape, a.dtype) for a in landed],
        in_specs=[anywhere] * len(landed),
        out_specs=[hbm] * len(landed),
        scratch_shapes=[dma((len(landed),))],
        compiler_params=pltpu.CompilerParams(vmem_limit_bytes=VMEM_FOR_REST),
        cost_estimate=pl.CostEstimate(
            flops=0, bytes_accessed=2 * sum(a.size for a in landed), transcendentals=0
        ),
    )(*landed)
    return gate.transpose(0, 2, 1), up.transpose(0, 2, 1), scale_gate, scale_up, router.T


def plain(master_gate, master_up, router_weight, router_gain):
    scale_gate, scale_up = lax.pmax(
        (jnp.max(jnp.abs(master_gate), axis=1), jnp.max(jnp.abs(master_up), axis=1)), "rows"
    )
    narrow_gate, narrow_up = (
        (master_gate / jnp.expand_dims(scale_gate, 1)).astype(jnp.bfloat16),
        (master_up / jnp.expand_dims(scale_up, 1)).astype(jnp.bfloat16),
    )
    final_gate, final_up = (
        lax.all_to_all(narrow_gate, "rows", split_axis=2, concat_axis=1, tiled=True),
        lax.all_to_all(narrow_up, "rows", split_axis=2, concat_axis=1, tiled=True),
    )
    scale_gate = lax.dynamic_slice_in_dim(
        scale_gate, lax.axis_index("rows") * final_gate.shape[2], final_gate.shape[2], axis=1
    )
    scale_up = lax.dynamic_slice_in_dim(
        scale_up, lax.axis_index("rows") * final_up.shape[2], final_up.shape[2], axis=1
    )
    part_router = (router_weight * router_gain[:, None]).astype(jnp.bfloat16)
    row_router = lax.all_gather(part_router, "rows", axis=0, tiled=True)
    serve_router = lax.all_gather(row_router, "owner", axis=1, tiled=True)
    return (final_gate, final_up, scale_gate, scale_up, serve_router)


def solution(mesh):
    owners, peers = mesh.shape["owner"], mesh.shape["rows"]

    def shards(master_gate, master_up, router_weight, router_gain):
        experts, rows, width = master_gate.shape
        whole_tiles = (
            peers & (peers - 1) == 0
            and peers > 2
            and rows % LANES == 0
            and width % LANES == 0
            and width % (peers * PACKED) == 0
            and experts % SUBLANES == 0
            and router_weight.shape[1] % PACKED == 0
            and (4 * experts + 4 * SLOTS) * rows * width <= VMEM_FOR_BLOCKS
        )
        run = functools.partial(fused, owners, peers) if whole_tiles else plain
        return run(master_gate, master_up, router_weight, router_gain)

    return jax.shard_map(
        shards,
        mesh=mesh,
        in_specs=(
            P("owner", "rows", None),
            P("owner", "rows", None),
            P("rows", "owner"),
            P("rows"),
        ),
        out_specs=(
            P("owner", None, "rows"),
            P("owner", None, "rows"),
            P("owner", "rows"),
            P("owner", "rows"),
            P(),
        ),
        check_vma=False,
    )
```

```python
import functools

import jax
import jax.numpy as jnp
from jax import lax
from jax.experimental import pallas as pl
from jax.experimental.pallas import tpu as pltpu
from jax.sharding import PartitionSpec as P

MESH = pl.DeviceIdType.MESH
LANES = 128
SUBLANES = 8
PACKED = 16
SLOTS = 5
DIRECT = 2
LATER = (0, 3)
LANDINGS = 4
VMEM_FOR_BLOCKS = 48 * 1024 * 1024
VMEM_FOR_REST = 2 * 1024 * 1024


def half(lower, tiles, far):
    count = -(-tiles // 2)
    if far:
        return jnp.where(lower, tiles - count, 0), count
    return jnp.where(lower, 0, count), tiles - count


def kernel(
    owners,
    peers,
    gate,
    up,
    router_hbm,
    gain_hbm,
    out_gate,
    out_up,
    out_router,
    out_scale_gate,
    out_scale_up,
    scales_rest,
    slots,
    seen,
    opening,
    largest_first,
    largest_rest,
    scales_first,
    parts_first,
    parts_rest,
    partial_first,
    partial_rest,
    across_first,
    across_rest,
    send,
    router,
    gain,
    row,
    slot_sem,
    small_sem,
    send_sem,
    recv_sem,
    seen_send,
    seen_recv,
    part_send,
    part_recv,
    across_send,
    across_recv,
    whole_send,
    whole_recv,
    router_send,
    router_recv,
):
    owner, me = lax.axis_index("owner"), lax.axis_index("rows")
    experts, rows, width = gate.shape
    tiles = width // LANES
    cut = width // peers
    near = peers // 2
    spot = lax.rem(me, near)
    masters, outs = (gate, up), (out_gate, out_up)
    largest, parts = (largest_first, largest_rest), (parts_first, parts_rest)
    partial, across = (partial_first, partial_rest), (across_first, across_rest)
    scales = (scales_first, scales_rest)
    lanes = pl.ds(pl.multiple_of(me * rows, LANES), rows)

    def partner(k):
        bits = [1 << b for b in range(peers.bit_length() - 1) if k >> b & 1]
        return sum((bit - 2 * bit * lax.rem(me // bit, 2) for bit in bits), me)

    def remote(src, dst, sent, received, to):
        return pltpu.make_async_remote_copy(
            src_ref=src,
            dst_ref=dst,
            send_sem=sent,
            recv_sem=received,
            device_id=to,
            device_id_type=MESH,
        )

    stream = [(0, 0, SUBLANES), (0, 0, DIRECT)]
    if experts > SUBLANES:
        stream.append((0, SUBLANES, experts - SUBLANES))
    stream += [(1, 0, experts), (0, DIRECT, experts - DIRECT)]
    stream.append((1, 0, experts - max(LATER)))
    bases = [sum(length for _, _, length in stream[:q]) for q in range(len(stream))]
    total = sum(length for _, _, length in stream)

    def fetch(m, e, i):
        s = lax.rem(i, SLOTS)
        return pltpu.make_async_copy(masters[m].at[e], slots.at[s], slot_sem.at[s])

    def fetch_start(i):
        for (m, first, length), base in zip(stream, bases):
            if isinstance(i, int):
                if base <= i < base + length:
                    fetch(m, first + i - base, i).start()
            else:

                @pl.when(jnp.logical_and(i >= base, i < base + length))
                def _():
                    fetch(m, first + i - base, i).start()

    def arrived(q, i):
        m, first, _ = stream[q]
        fetch(m, first + i, bases[q] + i).wait()
        return first + i, lax.rem(bases[q] + i, SLOTS)

    def following(q, i, steps):
        ahead = bases[q] + i + SLOTS
        low = bases[q] + SLOTS
        for (m, first, length), base in zip(stream, bases):
            if base + length <= low or base >= low + steps:
                continue
            if base <= low and base + length >= low + steps:
                fetch(m, first + ahead - base, ahead).start()
            else:

                @pl.when(jnp.logical_and(ahead >= base, ahead < base + length))
                def _():
                    fetch(m, first + ahead - base, ahead).start()

    def spots(m, e, c, first):
        k = m * experts + e - (0 if first else SUBLANES)
        return (k // SUBLANES) * tiles + c, pl.ds(k % SUBLANES if isinstance(k, int) else lax.rem(k, SUBLANES), 1)

    def measure(m, e, s, first):
        found = []
        for c in range(tiles):
            x = slots[s, :, c * LANES : (c + 1) * LANES]
            tile, sub = spots(m, e, c, first)
            found.append(jnp.max(jnp.abs(x), axis=0, keepdims=True))
            largest[0 if first else 1][tile, sub, :] = found[-1]
        return found

    def maxima(q, start, first):
        m, _, length = stream[q]

        def body(i, _):
            e, s = arrived(q, i)
            measure(m, e, s, first)
            following(q, i, length)
            return 0

        lax.fori_loop(start, length, body, 0)

    def seen_copy(e, k):
        return remote(
            seen.at[e, 0, pl.ds(0, tiles)],
            seen.at[e, k, pl.ds(0, tiles)],
            seen_send.at[e, k],
            seen_recv.at[e, k],
            {"rows": partner(k)},
        )

    def part_copy(stage, k):
        per = parts[stage].shape[1]
        to = partner(k)
        return remote(
            largest[stage].at[pl.ds(lax.rem(to, near) * per, per)],
            parts[stage].at[k],
            part_send.at[stage, k],
            part_recv.at[stage, k],
            {"rows": to},
        )

    def across_copy(stage):
        return remote(
            partial[stage],
            across[stage],
            across_send.at[stage],
            across_recv.at[stage],
            {"rows": partner(near)},
        )

    def share(stage, of):
        per = parts[stage].shape[1]
        return scales[stage].at[pl.ds(of * per, per)]

    def whole_copy(stage, k):
        return remote(
            share(stage, spot),
            share(stage, spot),
            whole_send.at[stage, k],
            whole_recv.at[stage, k],
            {"rows": partner(k)},
        )

    def scatter(stage):
        for k in range(1, near):
            part_copy(stage, k).start()

    def reduce(stage):
        per = parts[stage].shape[1]
        most = largest[stage][pl.ds(spot * per, per)]
        for k in range(1, near):
            part_copy(stage, k).wait_recv()
            most = jnp.maximum(most, parts[stage][k])
        partial[stage][...] = most
        across_copy(stage).start()

    def spread(stage):
        across_copy(stage).wait_recv()
        share(stage, spot)[...] = jnp.maximum(partial[stage][...], across[stage][...])
        for k in range(1, near):
            whole_copy(stage, k).start()

    def gathered(stage):
        across_copy(stage).wait_send()
        for k in range(1, near):
            part_copy(stage, k).wait_send()
            there = share(stage, lax.rem(partner(k), near))
            pltpu.make_async_copy(there, there, whole_recv.at[stage, k]).wait()
            whole_copy(stage, k).wait_send()

    def send_copy(m, k, e, length):
        to = partner(k)
        return remote(
            send.at[m, pl.ds(e, length), pl.ds(pl.multiple_of(to * cut, PACKED), cut), :],
            outs[m].at[pl.ds(e, length), :, lanes],
            send_sem.at[m, k],
            recv_sem.at[m, k],
            {"rows": to},
        )

    def keep_copy(m, e, length):
        return pltpu.make_async_copy(
            send.at[m, pl.ds(e, length), pl.ds(pl.multiple_of(me * cut, PACKED), cut), :],
            outs[m].at[pl.ds(e, length), :, lanes],
            send_sem.at[m, 0],
        )

    held = range(near + near // 2, peers)

    def one(m, e, s, scale_of, hold=False):
        for far in (True, False):
            low, count = half(me < near, tiles, far)
            for c in range(count):
                at = pl.ds(pl.multiple_of((low + c) * LANES, LANES), LANES)
                send[m, e, at, :] = (slots[s, :, at] / scale_of(low + c)).T.astype(send.dtype)
            for k in range(near, peers) if far else range(1, near):
                if not (hold and k in held):
                    send_copy(m, k, e, 1).start()
        keep_copy(m, e, 1).start()

    def bulk(q, start, stop, first):
        m, _, _ = stream[q]

        def body(i, _):
            e, s = arrived(q, i)

            def scale_of(c):
                tile, sub = spots(m, e, c, first)
                return scales[0 if first else 1][tile, sub, :]

            one(m, e, s, scale_of)
            following(q, i, stream[q][2])
            return 0

        lax.fori_loop(start, stop, body, 0)

    def early(q, i, hold):
        e = stream[q][1] + i
        for k in range(1, peers):
            seen_copy(e, k).wait_recv()
        opening[e, :tiles, :] = jnp.max(seen[e, :, :tiles, :], axis=0)
        _, s = arrived(q, i)
        one(0, e, s, lambda c: opening[e, pl.ds(c, 1), :], hold)
        fetch_start(bases[q] + i + SLOTS)

    depth = router.shape[0]
    mine = pl.ds(pl.multiple_of(owner * depth, PACKED), depth)

    def block(of):
        return out_router.at[mine, pl.ds(pl.multiple_of(of * rows, LANES), rows)]

    def router_across():
        return remote(row, block(me), router_send.at[0], router_recv.at[0], {"rows": partner(near)})

    def router_near(k, far):
        of = partner(near) if far else me
        return remote(
            block(of) if far else row,
            block(of),
            router_send.at[1 + 2 * k + far],
            router_recv.at[1 + 2 * k + far],
            {"rows": partner(k)},
        )

    def router_near_arrival(k, far):
        there = block(partner(near + k) if far else partner(k))
        return pltpu.make_async_copy(there, there, router_recv.at[1 + 2 * k + far])

    def router_owner(j):
        return remote(
            out_router.at[mine],
            out_router.at[mine],
            router_send.at[peers + j],
            router_recv.at[peers + j],
            {"owner": lax.rem(owner + j, owners)},
        )

    def router_owner_arrival(j):
        from_owner = lax.rem(owner + owners - j, owners)
        there = out_router.at[pl.ds(pl.multiple_of(from_owner * depth, PACKED), depth)]
        return pltpu.make_async_copy(there, there, router_recv.at[peers + j])

    barrier = pltpu.get_barrier_semaphore()

    fetch_start(0)
    for k in range(1, peers):
        pl.semaphore_signal(barrier, inc=1, device_id={"rows": partner(k)}, device_id_type=MESH)
    for j in range(1, owners):
        pl.semaphore_signal(
            barrier,
            inc=1,
            device_id={"owner": lax.rem(owner + j, owners)},
            device_id_type=MESH,
        )
    smalls = [
        pltpu.make_async_copy(router_hbm, router, small_sem.at[0]),
        pltpu.make_async_copy(gain_hbm, gain, small_sem.at[1]),
    ]
    largest_first[...] = jnp.zeros_like(largest_first)
    largest_rest[...] = jnp.zeros_like(largest_rest)
    for e in range(DIRECT):
        _, s = arrived(0, e)
        if e == 0:
            for i in range(1, SLOTS):
                fetch_start(i)
        found = measure(0, e, s, True)
        for c in range(tiles):
            seen[e, 0, c : c + 1, :] = found[c]
        if e == 0:
            for copy in smalls:
                copy.start()
            pl.semaphore_wait(barrier, peers - 1 + owners - 1)
        for k in range(1, peers):
            seen_copy(e, k).start()
        fetch_start(e + SLOTS)
    for copy in smalls:
        copy.wait()
    row[...] = (router[...] * gain[...]).astype(row.dtype)
    router_across().start()
    keep_router = pltpu.make_async_copy(row, block(me), small_sem.at[0])
    keep_router.start()
    maxima(0, DIRECT, True)
    scatter(0)
    early(1, 0, False)
    reduce(0)
    early(1, 1, True)
    rest = 2
    if experts > SUBLANES:
        maxima(rest, 0, False)
        rest += 1
    maxima(rest, 0, False)
    rest += 1
    router_across().wait_recv()
    for k in range(1, near):
        router_near(k, 0).start()
        router_near(k, 1).start()
    spread(0)
    scatter(1)
    for k in held:
        send_copy(0, k, 1, 1).start()
    gathered(0)
    bulk(rest, 0, 1, True)
    reduce(1)
    bulk(rest, 1, 2, True)
    spread(1)
    bulk(rest, 2, SUBLANES - DIRECT, True)
    gathered(1)
    if experts > SUBLANES:
        bulk(rest, SUBLANES - DIRECT, experts - DIRECT, False)
    keep_router.wait()
    router_across().wait_send()
    for k in range(1, near):
        for far in range(2):
            router_near_arrival(k, far).wait()
            router_near(k, far).wait_send()
    for j in range(1, owners):
        router_owner(j).start()
    bulk(rest + 1, 0, experts - max(LATER), False)
    for turn, later in enumerate(LATER):
        if later == max(LATER):
            continue

        @pl.when(lax.rem(owner, len(LATER)) == turn)
        def _():
            extra = max(LATER) - later
            low = experts - max(LATER)
            for i in range(extra):
                fetch(1, low + i, i).start()

            def body(i, _):
                fetch(1, low + i, i).wait()

                def scale_of(c):
                    tile, sub = spots(1, low + i, c, False)
                    return scales_rest[tile, sub, :]

                one(1, low + i, i, scale_of)
                return 0

            lax.fori_loop(0, extra, body, 0)


    for at in range(peers):

        @pl.when(me == at)
        def _():
            low = at * cut // LANES
            high = -(-(at + 1) * cut // LANES)
            for m in range(2):
                for e in range(0, experts, SUBLANES):
                    first = m == 0 and e == 0
                    found = []
                    for c in range(low, high):
                        k = m * experts + e - (0 if first else SUBLANES)
                        found.append(scales[0 if first else 1][(k // SUBLANES) * tiles + c])
                    found = jnp.concatenate(found, axis=1)
                    begin = at * cut - low * LANES
                    out = (out_scale_gate, out_scale_up)[m]
                    out[e : e + SUBLANES, :] = found[:, begin : begin + cut]

    for e in range(DIRECT):
        for k in range(1, peers):
            seen_copy(e, k).wait_send()
    for j in range(1, owners):
        router_owner_arrival(j).wait()
        router_owner(j).wait_send()
    keep_copy(0, 0, experts).wait()
    for k in range(1, peers):
        send_copy(0, k, 0, experts).wait()
    for turn, later in enumerate(LATER):

        @pl.when(lax.rem(owner, len(LATER)) == turn)
        def _():
            keep_copy(1, 0, experts - later).wait()
            for k in range(1, peers):
                send_copy(1, k, 0, experts - later).wait()


def last_kernel(peers, up, scales, out, slots, send, slot_sem, send_sem, recv_sem):
    owner, me = lax.axis_index("owner"), lax.axis_index("rows")
    experts, rows, width = up.shape
    tiles = width // LANES
    cut = width // peers
    lanes = pl.ds(pl.multiple_of(me * rows, LANES), rows)
    turn = lax.rem(owner, len(LATER))
    later = sum(jnp.where(turn == t, n, 0) for t, n in enumerate(LATER))

    def partner(k):
        bits = [1 << b for b in range(peers.bit_length() - 1) if k >> b & 1]
        return sum((bit - 2 * bit * lax.rem(me // bit, 2) for bit in bits), me)

    def fetch(i):
        return pltpu.make_async_copy(
            up.at[experts - later + i], slots.at[i], slot_sem.at[i]
        )

    def prepare(i):
        fetch(i).wait()
        sub = pl.ds(SUBLANES - later + i, 1)
        for c in range(tiles):
            x = slots[i, :, c * LANES : (c + 1) * LANES]
            send[i, c * LANES : (c + 1) * LANES, :] = (x / scales[c, sub, :]).T.astype(send.dtype)

    def send_copy(k, i, length):
        to = partner(k)
        return pltpu.make_async_remote_copy(
            src_ref=send.at[pl.ds(i, length), pl.ds(pl.multiple_of(to * cut, PACKED), cut), :],
            dst_ref=out.at[pl.ds(i, length), :, lanes],
            send_sem=send_sem.at[k],
            recv_sem=recv_sem.at[k],
            device_id={"rows": to},
            device_id_type=MESH,
        )

    def keep_copy(i, length):
        return pltpu.make_async_copy(
            send.at[pl.ds(i, length), pl.ds(pl.multiple_of(me * cut, PACKED), cut), :],
            out.at[pl.ds(i, length), :, lanes],
            send_sem.at[0],
        )

    def post(i):
        for k in range(1, peers):
            send_copy(k, i, 1).start()
        keep_copy(i, 1).start()

    barrier = pltpu.get_barrier_semaphore()
    for k in range(1, peers):
        pl.semaphore_signal(barrier, inc=1, device_id={"rows": partner(k)}, device_id_type=MESH)

    def begin(i, _):
        fetch(i).start()
        return 0

    lax.fori_loop(0, later, begin, 0)
    if min(LATER) > 0:
        prepare(0)
    else:
        pl.when(later > 0)(lambda: prepare(0))
    pl.semaphore_wait(barrier, peers - 1)
    if min(LATER) > 0:
        post(0)
    else:
        pl.when(later > 0)(lambda: post(0))

    def body(i, _):
        prepare(i)
        post(i)
        return 0

    lax.fori_loop(1, later, body, 0)
    for t, n in enumerate(LATER):
        if n == 0:
            continue

        @pl.when(turn == t)
        def _():
            keep_copy(0, n).wait()
            for k in range(1, peers):
                send_copy(k, 0, n).wait()


def land(gate, up, router, scale_gate, scale_up, scales, *refs):
    outs, last_scales, sem = refs[:5], refs[5], refs[6]
    tiles = last_scales.shape[0]
    experts = gate.shape[0]

    def move(i, a, b, low, high, pieces):
        cuts = [low + (high - low) * j // pieces for j in range(pieces + 1)]
        for at, end in zip(cuts, cuts[1:]):
            span = pl.ds(at, end - at)
            pltpu.make_async_copy(a.at[span], b.at[span], sem.at[i]).start()

    def moved(i, a, b, low, high):
        span = pl.ds(low, high - low)
        pltpu.make_async_copy(a.at[span], b.at[span], sem.at[i]).wait()

    whole = [(0, gate), (2, router), (3, scale_gate), (4, scale_up)]
    for i, a in whole:
        move(i, a, outs[i], 0, a.shape[0], LANDINGS if i == 0 else 1)
    for turn, later in enumerate(LATER):

        @pl.when(lax.rem(lax.axis_index("owner"), len(LATER)) == turn)
        def _():
            move(1, up, outs[1], 0, experts - later, LANDINGS)
            moved(1, up, outs[1], 0, experts - later)

    low = (2 * experts // SUBLANES - 2) * tiles
    last_scales[...] = scales[low : low + tiles]
    for i, a in whole:
        moved(i, a, outs[i], 0, a.shape[0])


def last_land(_, last, up, sem):
    experts = up.shape[0]
    for turn, later in enumerate(LATER):
        if later == 0:
            continue

        @pl.when(lax.rem(lax.axis_index("owner"), len(LATER)) == turn)
        def _():
            there = up.at[pl.ds(experts - later, later)]
            copy = pltpu.make_async_copy(last.at[pl.ds(0, later)], there, sem)
            copy.start()
            copy.wait()


def fused(owners, peers, master_gate, master_up, router_weight, router_gain):
    experts, rows, width = master_gate.shape
    cut = width // peers
    near = peers // 2
    tiles = width // LANES
    padded = -(-tiles // SUBLANES) * SUBLANES
    groups = 2 * experts // SUBLANES
    first, rest = -(-tiles // near), -(-(groups - 1) * tiles // near)
    depth = router_weight.shape[1]
    anywhere = pl.BlockSpec(memory_space=pl.ANY)
    vmem = pl.BlockSpec(memory_space=pltpu.VMEM)
    hbm = pl.BlockSpec(memory_space=pltpu.HBM)
    dma = pltpu.SemaphoreType.DMA
    turned = jax.ShapeDtypeStruct((experts, cut, rows * peers), jnp.bfloat16)
    scale = jax.ShapeDtypeStruct((experts, cut), jnp.float32)

    def in_hbm(a):
        return pltpu.with_memory_space_constraint(a, pltpu.HBM)

    def maxima(*shape):
        return pltpu.VMEM((*shape, SUBLANES, LANES), jnp.float32)

    landed = pl.pallas_call(
        functools.partial(kernel, owners, peers),
        out_shape=(
            turned,
            turned,
            jax.ShapeDtypeStruct((depth * owners, rows * peers), jnp.bfloat16),
            scale,
            scale,
            jax.ShapeDtypeStruct((rest * near, SUBLANES, LANES), jnp.float32),
        ),
        in_specs=[anywhere, anywhere, hbm, hbm],
        out_specs=(anywhere, anywhere, anywhere, vmem, vmem, vmem),
        scratch_shapes=[
            pltpu.VMEM((SLOTS, rows, width), jnp.float32),
            pltpu.VMEM((DIRECT, peers, padded, LANES), jnp.float32),
            pltpu.VMEM((DIRECT, padded, LANES), jnp.float32),
            maxima(first * near),
            maxima(rest * near),
            maxima(first * near),
            maxima(near, first),
            maxima(near, rest),
            maxima(first),
            maxima(rest),
            maxima(first),
            maxima(rest),
            pltpu.VMEM((2, experts, width, rows), jnp.bfloat16),
            pltpu.VMEM((depth, rows), jnp.float32),
            pltpu.VMEM((1, rows), jnp.float32),
            pltpu.VMEM((depth, rows), jnp.bfloat16),
            dma((SLOTS,)),
            dma((2,)),
            dma((2, peers)),
            dma((2, peers)),
            dma((DIRECT, peers)),
            dma((DIRECT, peers)),
            dma((2, near)),
            dma((2, near)),
            dma((2,)),
            dma((2,)),
            dma((2, near)),
            dma((2, near)),
            dma((peers + owners,)),
            dma((peers + owners,)),
        ],
        compiler_params=pltpu.CompilerParams(
            collective_id=0,
            has_side_effects=True,
            vmem_limit_bytes=(4 * experts + 4 * SLOTS) * rows * width + VMEM_FOR_REST,
        ),
    )(*(in_hbm(a) for a in (master_gate, master_up, router_weight.T, router_gain[None, :])))
    local = [jax.ShapeDtypeStruct(a.shape, a.dtype) for a in landed[:5]]
    small = pltpu.CompilerParams(vmem_limit_bytes=VMEM_FOR_REST)
    gate, up, router, scale_gate, scale_up, scales = pl.pallas_call(
        land,
        out_shape=[*local, jax.ShapeDtypeStruct((tiles, SUBLANES, LANES), jnp.float32)],
        in_specs=[anywhere] * 5 + [vmem],
        out_specs=[hbm] * 5 + [vmem],
        scratch_shapes=[dma((5,))],
        compiler_params=small,
    )(*landed)
    most = max(LATER)
    last = pl.pallas_call(
        functools.partial(last_kernel, peers),
        out_shape=jax.ShapeDtypeStruct((most, cut, rows * peers), jnp.bfloat16),
        in_specs=[anywhere, vmem],
        out_specs=anywhere,
        scratch_shapes=[
            pltpu.VMEM((most, rows, width), jnp.float32),
            pltpu.VMEM((most, width, rows), jnp.bfloat16),
            dma((most,)),
            dma((peers,)),
            dma((peers,)),
        ],
        compiler_params=pltpu.CompilerParams(
            collective_id=1,
            has_side_effects=True,
            vmem_limit_bytes=6 * most * rows * width + VMEM_FOR_REST,
        ),
    )(in_hbm(master_up), scales)
    up = pl.pallas_call(
        last_land,
        out_shape=local[1],
        in_specs=[hbm, anywhere],
        out_specs=hbm,
        scratch_shapes=[dma],
        input_output_aliases={0: 0},
        compiler_params=small,
    )(up, last)
    return gate.transpose(0, 2, 1), up.transpose(0, 2, 1), scale_gate, scale_up, router.T


def plain(master_gate, master_up, router_weight, router_gain):
    scale_gate, scale_up = lax.pmax(
        (jnp.max(jnp.abs(master_gate), axis=1), jnp.max(jnp.abs(master_up), axis=1)), "rows"
    )
    narrow_gate, narrow_up = (
        (master_gate / jnp.expand_dims(scale_gate, 1)).astype(jnp.bfloat16),
        (master_up / jnp.expand_dims(scale_up, 1)).astype(jnp.bfloat16),
    )
    final_gate, final_up = (
        lax.all_to_all(narrow_gate, "rows", split_axis=2, concat_axis=1, tiled=True),
        lax.all_to_all(narrow_up, "rows", split_axis=2, concat_axis=1, tiled=True),
    )
    scale_gate = lax.dynamic_slice_in_dim(
        scale_gate, lax.axis_index("rows") * final_gate.shape[2], final_gate.shape[2], axis=1
    )
    scale_up = lax.dynamic_slice_in_dim(
        scale_up, lax.axis_index("rows") * final_up.shape[2], final_up.shape[2], axis=1
    )
    part_router = (router_weight * router_gain[:, None]).astype(jnp.bfloat16)
    row_router = lax.all_gather(part_router, "rows", axis=0, tiled=True)
    serve_router = lax.all_gather(row_router, "owner", axis=1, tiled=True)
    return (final_gate, final_up, scale_gate, scale_up, serve_router)


def solution(mesh):
    owners, peers = mesh.shape["owner"], mesh.shape["rows"]

    def shards(master_gate, master_up, router_weight, router_gain):
        experts, rows, width = master_gate.shape
        whole_tiles = (
            peers & (peers - 1) == 0
            and peers > 2
            and rows % LANES == 0
            and width % LANES == 0
            and width % (peers * PACKED) == 0
            and experts % SUBLANES == 0
            and router_weight.shape[1] % PACKED == 0
            and (4 * experts + 4 * SLOTS) * rows * width <= VMEM_FOR_BLOCKS
        )
        run = functools.partial(fused, owners, peers) if whole_tiles else plain
        return run(master_gate, master_up, router_weight, router_gain)

    return jax.shard_map(
        shards,
        mesh=mesh,
        in_specs=(
            P("owner", "rows", None),
            P("owner", "rows", None),
            P("rows", "owner"),
            P("rows"),
        ),
        out_specs=(
            P("owner", None, "rows"),
            P("owner", None, "rows"),
            P("owner", "rows"),
            P("owner", "rows"),
            P(),
        ),
        check_vma=False,
    )
```

```python
import functools

import jax
import jax.numpy as jnp
from jax import lax
from jax.experimental import pallas as pl
from jax.experimental.pallas import tpu as pltpu
from jax.sharding import PartitionSpec as P

MESH = pl.DeviceIdType.MESH
LANES = 128
SUBLANES = 8
PACKED = 16
SLOTS = 5
DIRECT = 2
LATER = (0, 3)
LANDINGS = 4
VMEM_FOR_BLOCKS = 48 * 1024 * 1024
VMEM_FOR_REST = 2 * 1024 * 1024


def half(lower, tiles, far):
    count = -(-tiles // 2)
    if far:
        return jnp.where(lower, tiles - count, 0), count
    return jnp.where(lower, 0, count), tiles - count


def far_targets(me, peers):
    near = peers // 2
    base = near - near * (me // near)
    return [base + p for p in range(near)]


def kernel(
    owners,
    peers,
    gate,
    up,
    router_hbm,
    gain_hbm,
    out_gate,
    out_up,
    out_router,
    out_scale_gate,
    out_scale_up,
    scales_rest,
    slots,
    seen,
    opening,
    largest_first,
    largest_rest,
    scales_first,
    parts_first,
    parts_rest,
    partial_first,
    partial_rest,
    across_first,
    across_rest,
    send,
    router,
    gain,
    row,
    slot_sem,
    small_sem,
    send_sem,
    recv_sem,
    seen_send,
    seen_recv,
    part_send,
    part_recv,
    across_send,
    across_recv,
    whole_send,
    whole_recv,
    router_send,
    router_recv,
):
    owner, me = lax.axis_index("owner"), lax.axis_index("rows")
    experts, rows, width = gate.shape
    tiles = width // LANES
    cut = width // peers
    near = peers // 2
    spot = lax.rem(me, near)
    masters, outs = (gate, up), (out_gate, out_up)
    largest, parts = (largest_first, largest_rest), (parts_first, parts_rest)
    partial, across = (partial_first, partial_rest), (across_first, across_rest)
    scales = (scales_first, scales_rest)
    lanes = pl.ds(pl.multiple_of(me * rows, LANES), rows)

    def partner(k):
        bits = [1 << b for b in range(peers.bit_length() - 1) if k >> b & 1]
        return sum((bit - 2 * bit * lax.rem(me // bit, 2) for bit in bits), me)

    def remote(src, dst, sent, received, to):
        return pltpu.make_async_remote_copy(
            src_ref=src,
            dst_ref=dst,
            send_sem=sent,
            recv_sem=received,
            device_id=to,
            device_id_type=MESH,
        )

    stream = [(0, 0, SUBLANES), (0, 0, DIRECT)]
    if experts > SUBLANES:
        stream.append((0, SUBLANES, experts - SUBLANES))
    stream += [(1, 0, experts), (0, DIRECT, experts - DIRECT)]
    stream.append((1, 0, experts - max(LATER)))
    bases = [sum(length for _, _, length in stream[:q]) for q in range(len(stream))]
    total = sum(length for _, _, length in stream)

    def fetch(m, e, i):
        s = lax.rem(i, SLOTS)
        return pltpu.make_async_copy(masters[m].at[e], slots.at[s], slot_sem.at[s])

    def fetch_start(i):
        for (m, first, length), base in zip(stream, bases):
            if isinstance(i, int):
                if base <= i < base + length:
                    fetch(m, first + i - base, i).start()
            else:

                @pl.when(jnp.logical_and(i >= base, i < base + length))
                def _():
                    fetch(m, first + i - base, i).start()

    def arrived(q, i):
        m, first, _ = stream[q]
        fetch(m, first + i, bases[q] + i).wait()
        return first + i, lax.rem(bases[q] + i, SLOTS)

    def following(q, i, steps):
        ahead = bases[q] + i + SLOTS
        low = bases[q] + SLOTS
        for (m, first, length), base in zip(stream, bases):
            if base + length <= low or base >= low + steps:
                continue
            if base <= low and base + length >= low + steps:
                fetch(m, first + ahead - base, ahead).start()
            else:

                @pl.when(jnp.logical_and(ahead >= base, ahead < base + length))
                def _():
                    fetch(m, first + ahead - base, ahead).start()

    def spots(m, e, c, first):
        k = m * experts + e - (0 if first else SUBLANES)
        return (k // SUBLANES) * tiles + c, pl.ds(k % SUBLANES if isinstance(k, int) else lax.rem(k, SUBLANES), 1)

    def measure(m, e, s, first):
        found = []
        for c in range(tiles):
            x = slots[s, :, c * LANES : (c + 1) * LANES]
            tile, sub = spots(m, e, c, first)
            found.append(jnp.max(jnp.abs(x), axis=0, keepdims=True))
            largest[0 if first else 1][tile, sub, :] = found[-1]
        return found

    def maxima(q, start, first):
        m, _, length = stream[q]

        def body(i, _):
            e, s = arrived(q, i)
            measure(m, e, s, first)
            following(q, i, length)
            return 0

        lax.fori_loop(start, length, body, 0)

    def seen_copy(e, k):
        return remote(
            seen.at[e, 0, pl.ds(0, tiles)],
            seen.at[e, k, pl.ds(0, tiles)],
            seen_send.at[e, k],
            seen_recv.at[e, k],
            {"rows": partner(k)},
        )

    def part_copy(stage, k):
        per = parts[stage].shape[1]
        to = partner(k)
        return remote(
            largest[stage].at[pl.ds(lax.rem(to, near) * per, per)],
            parts[stage].at[k],
            part_send.at[stage, k],
            part_recv.at[stage, k],
            {"rows": to},
        )

    def across_copy(stage):
        return remote(
            partial[stage],
            across[stage],
            across_send.at[stage],
            across_recv.at[stage],
            {"rows": partner(near)},
        )

    def share(stage, of):
        per = parts[stage].shape[1]
        return scales[stage].at[pl.ds(of * per, per)]

    def whole_copy(stage, k):
        return remote(
            share(stage, spot),
            share(stage, spot),
            whole_send.at[stage, k],
            whole_recv.at[stage, k],
            {"rows": partner(k)},
        )

    def scatter(stage):
        for k in range(1, near):
            part_copy(stage, k).start()

    def reduce(stage):
        per = parts[stage].shape[1]
        most = largest[stage][pl.ds(spot * per, per)]
        for k in range(1, near):
            part_copy(stage, k).wait_recv()
            most = jnp.maximum(most, parts[stage][k])
        partial[stage][...] = most
        across_copy(stage).start()

    def spread(stage):
        across_copy(stage).wait_recv()
        share(stage, spot)[...] = jnp.maximum(partial[stage][...], across[stage][...])
        for k in range(1, near):
            whole_copy(stage, k).start()

    def gathered(stage):
        across_copy(stage).wait_send()
        for k in range(1, near):
            part_copy(stage, k).wait_send()
            there = share(stage, lax.rem(partner(k), near))
            pltpu.make_async_copy(there, there, whole_recv.at[stage, k]).wait()
            whole_copy(stage, k).wait_send()

    def send_copy(m, to, e, length):
        return remote(
            send.at[m, pl.ds(e, length), pl.ds(pl.multiple_of(to * cut, PACKED), cut), :],
            outs[m].at[pl.ds(e, length), :, lanes],
            send_sem.at[m, to],
            recv_sem.at[m, me],
            {"rows": to},
        )

    def sent_and_received(m, length):
        for to in [partner(k) for k in range(1, peers)]:
            send_copy(m, to, 0, length).wait_send()
            there = outs[m].at[pl.ds(0, length), :, pl.ds(pl.multiple_of(to * rows, LANES), rows)]
            pltpu.make_async_copy(there, there, recv_sem.at[m, to]).wait()

    def keep_copy(m, e, length):
        return pltpu.make_async_copy(
            send.at[m, pl.ds(e, length), pl.ds(pl.multiple_of(me * cut, PACKED), cut), :],
            outs[m].at[pl.ds(e, length), :, lanes],
            send_sem.at[m, me],
        )

    across_from = far_targets(me, peers)
    held = across_from[near // 2 :]

    def one(m, e, s, scale_of, hold=False):
        for far in (True, False):
            low, count = half(me < near, tiles, far)
            for c in range(count):
                at = pl.ds(pl.multiple_of((low + c) * LANES, LANES), LANES)
                send[m, e, at, :] = (slots[s, :, at] / scale_of(low + c)).T.astype(send.dtype)
            targets = [partner(k) for k in range(1, near)]
            if far:
                targets = across_from[: near // 2] if hold else across_from
            for to in targets:
                send_copy(m, to, e, 1).start()
        keep_copy(m, e, 1).start()

    def bulk(q, start, stop, first):
        m, _, _ = stream[q]

        def body(i, _):
            e, s = arrived(q, i)

            def scale_of(c):
                tile, sub = spots(m, e, c, first)
                return scales[0 if first else 1][tile, sub, :]

            one(m, e, s, scale_of)
            following(q, i, stream[q][2])
            return 0

        lax.fori_loop(start, stop, body, 0)

    def early(q, i, hold):
        e = stream[q][1] + i
        for k in range(1, peers):
            seen_copy(e, k).wait_recv()
        opening[e, :tiles, :] = jnp.max(seen[e, :, :tiles, :], axis=0)
        _, s = arrived(q, i)
        one(0, e, s, lambda c: opening[e, pl.ds(c, 1), :], hold)
        fetch_start(bases[q] + i + SLOTS)

    depth = router.shape[0]
    mine = pl.ds(pl.multiple_of(owner * depth, PACKED), depth)

    def block(of):
        return out_router.at[mine, pl.ds(pl.multiple_of(of * rows, LANES), rows)]

    def router_across():
        return remote(row, block(me), router_send.at[0], router_recv.at[0], {"rows": partner(near)})

    def router_near(k, far):
        of = partner(near) if far else me
        return remote(
            block(of) if far else row,
            block(of),
            router_send.at[1 + 2 * k + far],
            router_recv.at[1 + 2 * k + far],
            {"rows": partner(k)},
        )

    def router_near_arrival(k, far):
        there = block(partner(near + k) if far else partner(k))
        return pltpu.make_async_copy(there, there, router_recv.at[1 + 2 * k + far])

    def router_owner(j):
        return remote(
            out_router.at[mine],
            out_router.at[mine],
            router_send.at[peers + j],
            router_recv.at[peers + j],
            {"owner": lax.rem(owner + j, owners)},
        )

    def router_owner_arrival(j):
        from_owner = lax.rem(owner + owners - j, owners)
        there = out_router.at[pl.ds(pl.multiple_of(from_owner * depth, PACKED), depth)]
        return pltpu.make_async_copy(there, there, router_recv.at[peers + j])

    barrier = pltpu.get_barrier_semaphore()

    fetch_start(0)
    for k in range(1, peers):
        pl.semaphore_signal(barrier, inc=1, device_id={"rows": partner(k)}, device_id_type=MESH)
    for j in range(1, owners):
        pl.semaphore_signal(
            barrier,
            inc=1,
            device_id={"owner": lax.rem(owner + j, owners)},
            device_id_type=MESH,
        )
    smalls = [
        pltpu.make_async_copy(router_hbm, router, small_sem.at[0]),
        pltpu.make_async_copy(gain_hbm, gain, small_sem.at[1]),
    ]
    largest_first[...] = jnp.zeros_like(largest_first)
    largest_rest[...] = jnp.zeros_like(largest_rest)
    for e in range(DIRECT):
        _, s = arrived(0, e)
        if e == 0:
            for i in range(1, SLOTS):
                fetch_start(i)
        found = measure(0, e, s, True)
        for c in range(tiles):
            seen[e, 0, c : c + 1, :] = found[c]
        if e == 0:
            for copy in smalls:
                copy.start()
            pl.semaphore_wait(barrier, peers - 1 + owners - 1)
        for k in range(1, peers):
            seen_copy(e, k).start()
        fetch_start(e + SLOTS)
    for copy in smalls:
        copy.wait()
    row[...] = (router[...] * gain[...]).astype(row.dtype)
    router_across().start()
    keep_router = pltpu.make_async_copy(row, block(me), small_sem.at[0])
    keep_router.start()
    maxima(0, DIRECT, True)
    scatter(0)
    early(1, 0, False)
    reduce(0)
    early(1, 1, True)
    rest = 2
    if experts > SUBLANES:
        maxima(rest, 0, False)
        rest += 1
    maxima(rest, 0, False)
    rest += 1
    router_across().wait_recv()
    for k in range(1, near):
        router_near(k, 0).start()
        router_near(k, 1).start()
    spread(0)
    scatter(1)
    for to in held:
        send_copy(0, to, 1, 1).start()
    gathered(0)
    bulk(rest, 0, 1, True)
    reduce(1)
    bulk(rest, 1, 2, True)
    spread(1)
    bulk(rest, 2, SUBLANES - DIRECT, True)
    gathered(1)
    if experts > SUBLANES:
        bulk(rest, SUBLANES - DIRECT, experts - DIRECT, False)
    keep_router.wait()
    router_across().wait_send()
    for k in range(1, near):
        for far in range(2):
            router_near_arrival(k, far).wait()
            router_near(k, far).wait_send()
    for j in range(1, owners):
        router_owner(j).start()
    bulk(rest + 1, 0, experts - max(LATER), False)
    for turn, later in enumerate(LATER):
        if later == max(LATER):
            continue

        @pl.when(lax.rem(owner, len(LATER)) == turn)
        def _():
            extra = max(LATER) - later
            low = experts - max(LATER)
            for i in range(extra):
                fetch(1, low + i, i).start()

            def body(i, _):
                fetch(1, low + i, i).wait()

                def scale_of(c):
                    tile, sub = spots(1, low + i, c, False)
                    return scales_rest[tile, sub, :]

                one(1, low + i, i, scale_of)
                return 0

            lax.fori_loop(0, extra, body, 0)


    for at in range(peers):

        @pl.when(me == at)
        def _():
            low = at * cut // LANES
            high = -(-(at + 1) * cut // LANES)
            for m in range(2):
                for e in range(0, experts, SUBLANES):
                    first = m == 0 and e == 0
                    found = []
                    for c in range(low, high):
                        k = m * experts + e - (0 if first else SUBLANES)
                        found.append(scales[0 if first else 1][(k // SUBLANES) * tiles + c])
                    found = jnp.concatenate(found, axis=1)
                    begin = at * cut - low * LANES
                    out = (out_scale_gate, out_scale_up)[m]
                    out[e : e + SUBLANES, :] = found[:, begin : begin + cut]

    for e in range(DIRECT):
        for k in range(1, peers):
            seen_copy(e, k).wait_send()
    for j in range(1, owners):
        router_owner_arrival(j).wait()
        router_owner(j).wait_send()
    keep_copy(0, 0, experts).wait()
    sent_and_received(0, experts)
    for turn, later in enumerate(LATER):

        @pl.when(lax.rem(owner, len(LATER)) == turn)
        def _():
            keep_copy(1, 0, experts - later).wait()
            sent_and_received(1, experts - later)


def last_kernel(peers, up, scales, out, slots, send, slot_sem, send_sem, recv_sem):
    owner, me = lax.axis_index("owner"), lax.axis_index("rows")
    experts, rows, width = up.shape
    tiles = width // LANES
    cut = width // peers
    lanes = pl.ds(pl.multiple_of(me * rows, LANES), rows)
    near = peers // 2
    turn = lax.rem(owner, len(LATER))
    later = sum(jnp.where(turn == t, n, 0) for t, n in enumerate(LATER))

    def partner(k):
        bits = [1 << b for b in range(peers.bit_length() - 1) if k >> b & 1]
        return sum((bit - 2 * bit * lax.rem(me // bit, 2) for bit in bits), me)

    def fetch(i):
        return pltpu.make_async_copy(
            up.at[experts - later + i], slots.at[i], slot_sem.at[i]
        )

    def prepare(i):
        fetch(i).wait()
        sub = pl.ds(SUBLANES - later + i, 1)
        for c in range(tiles):
            x = slots[i, :, c * LANES : (c + 1) * LANES]
            send[i, c * LANES : (c + 1) * LANES, :] = (x / scales[c, sub, :]).T.astype(send.dtype)

    def send_copy(to, i, length):
        return pltpu.make_async_remote_copy(
            src_ref=send.at[pl.ds(i, length), pl.ds(pl.multiple_of(to * cut, PACKED), cut), :],
            dst_ref=out.at[pl.ds(i, length), :, lanes],
            send_sem=send_sem.at[to],
            recv_sem=recv_sem.at[me],
            device_id={"rows": to},
            device_id_type=MESH,
        )

    def keep_copy(i, length):
        return pltpu.make_async_copy(
            send.at[pl.ds(i, length), pl.ds(pl.multiple_of(me * cut, PACKED), cut), :],
            out.at[pl.ds(i, length), :, lanes],
            send_sem.at[me],
        )

    def post(i):
        for k in range(1, near):
            send_copy(partner(k), i, 1).start()
        for to in far_targets(me, peers):
            send_copy(to, i, 1).start()
        keep_copy(i, 1).start()

    barrier = pltpu.get_barrier_semaphore()
    for k in range(1, peers):
        pl.semaphore_signal(barrier, inc=1, device_id={"rows": partner(k)}, device_id_type=MESH)

    def begin(i, _):
        fetch(i).start()
        return 0

    lax.fori_loop(0, later, begin, 0)
    if min(LATER) > 0:
        prepare(0)
    else:
        pl.when(later > 0)(lambda: prepare(0))
    pl.semaphore_wait(barrier, peers - 1)
    if min(LATER) > 0:
        post(0)
    else:
        pl.when(later > 0)(lambda: post(0))

    def body(i, _):
        prepare(i)
        post(i)
        return 0

    lax.fori_loop(1, later, body, 0)
    for t, n in enumerate(LATER):
        if n == 0:
            continue

        @pl.when(turn == t)
        def _():
            keep_copy(0, n).wait()
            for to in [partner(k) for k in range(1, peers)]:
                send_copy(to, 0, n).wait_send()
                there = out.at[pl.ds(0, n), :, pl.ds(pl.multiple_of(to * rows, LANES), rows)]
                pltpu.make_async_copy(there, there, recv_sem.at[to]).wait()


def land(gate, up, router, scale_gate, scale_up, scales, *refs):
    outs, last_scales, sem = refs[:5], refs[5], refs[6]
    tiles = last_scales.shape[0]
    experts = gate.shape[0]

    def move(i, a, b, low, high, pieces):
        cuts = [low + (high - low) * j // pieces for j in range(pieces + 1)]
        for at, end in zip(cuts, cuts[1:]):
            span = pl.ds(at, end - at)
            pltpu.make_async_copy(a.at[span], b.at[span], sem.at[i]).start()

    def moved(i, a, b, low, high):
        span = pl.ds(low, high - low)
        pltpu.make_async_copy(a.at[span], b.at[span], sem.at[i]).wait()

    whole = [(0, gate), (2, router), (3, scale_gate), (4, scale_up)]
    for i, a in whole:
        move(i, a, outs[i], 0, a.shape[0], LANDINGS if i == 0 else 1)
    for turn, later in enumerate(LATER):

        @pl.when(lax.rem(lax.axis_index("owner"), len(LATER)) == turn)
        def _():
            move(1, up, outs[1], 0, experts - later, LANDINGS)
            moved(1, up, outs[1], 0, experts - later)

    low = (2 * experts // SUBLANES - 2) * tiles
    last_scales[...] = scales[low : low + tiles]
    for i, a in whole:
        moved(i, a, outs[i], 0, a.shape[0])


def last_land(_, last, up, sem):
    experts = up.shape[0]
    for turn, later in enumerate(LATER):
        if later == 0:
            continue

        @pl.when(lax.rem(lax.axis_index("owner"), len(LATER)) == turn)
        def _():
            there = up.at[pl.ds(experts - later, later)]
            copy = pltpu.make_async_copy(last.at[pl.ds(0, later)], there, sem)
            copy.start()
            copy.wait()


def fused(owners, peers, master_gate, master_up, router_weight, router_gain):
    experts, rows, width = master_gate.shape
    cut = width // peers
    near = peers // 2
    tiles = width // LANES
    padded = -(-tiles // SUBLANES) * SUBLANES
    groups = 2 * experts // SUBLANES
    first, rest = -(-tiles // near), -(-(groups - 1) * tiles // near)
    depth = router_weight.shape[1]
    anywhere = pl.BlockSpec(memory_space=pl.ANY)
    vmem = pl.BlockSpec(memory_space=pltpu.VMEM)
    hbm = pl.BlockSpec(memory_space=pltpu.HBM)
    dma = pltpu.SemaphoreType.DMA
    turned = jax.ShapeDtypeStruct((experts, cut, rows * peers), jnp.bfloat16)
    scale = jax.ShapeDtypeStruct((experts, cut), jnp.float32)

    def in_hbm(a):
        return pltpu.with_memory_space_constraint(a, pltpu.HBM)

    def maxima(*shape):
        return pltpu.VMEM((*shape, SUBLANES, LANES), jnp.float32)

    landed = pl.pallas_call(
        functools.partial(kernel, owners, peers),
        out_shape=(
            turned,
            turned,
            jax.ShapeDtypeStruct((depth * owners, rows * peers), jnp.bfloat16),
            scale,
            scale,
            jax.ShapeDtypeStruct((rest * near, SUBLANES, LANES), jnp.float32),
        ),
        in_specs=[anywhere, anywhere, hbm, hbm],
        out_specs=(anywhere, anywhere, anywhere, vmem, vmem, vmem),
        scratch_shapes=[
            pltpu.VMEM((SLOTS, rows, width), jnp.float32),
            pltpu.VMEM((DIRECT, peers, padded, LANES), jnp.float32),
            pltpu.VMEM((DIRECT, padded, LANES), jnp.float32),
            maxima(first * near),
            maxima(rest * near),
            maxima(first * near),
            maxima(near, first),
            maxima(near, rest),
            maxima(first),
            maxima(rest),
            maxima(first),
            maxima(rest),
            pltpu.VMEM((2, experts, width, rows), jnp.bfloat16),
            pltpu.VMEM((depth, rows), jnp.float32),
            pltpu.VMEM((1, rows), jnp.float32),
            pltpu.VMEM((depth, rows), jnp.bfloat16),
            dma((SLOTS,)),
            dma((2,)),
            dma((2, peers)),
            dma((2, peers)),
            dma((DIRECT, peers)),
            dma((DIRECT, peers)),
            dma((2, near)),
            dma((2, near)),
            dma((2,)),
            dma((2,)),
            dma((2, near)),
            dma((2, near)),
            dma((peers + owners,)),
            dma((peers + owners,)),
        ],
        compiler_params=pltpu.CompilerParams(
            collective_id=0,
            has_side_effects=True,
            vmem_limit_bytes=(4 * experts + 4 * SLOTS) * rows * width + VMEM_FOR_REST,
        ),
    )(*(in_hbm(a) for a in (master_gate, master_up, router_weight.T, router_gain[None, :])))
    local = [jax.ShapeDtypeStruct(a.shape, a.dtype) for a in landed[:5]]
    small = pltpu.CompilerParams(vmem_limit_bytes=VMEM_FOR_REST)
    gate, up, router, scale_gate, scale_up, scales = pl.pallas_call(
        land,
        out_shape=[*local, jax.ShapeDtypeStruct((tiles, SUBLANES, LANES), jnp.float32)],
        in_specs=[anywhere] * 5 + [vmem],
        out_specs=[hbm] * 5 + [vmem],
        scratch_shapes=[dma((5,))],
        compiler_params=small,
    )(*landed)
    most = max(LATER)
    last = pl.pallas_call(
        functools.partial(last_kernel, peers),
        out_shape=jax.ShapeDtypeStruct((most, cut, rows * peers), jnp.bfloat16),
        in_specs=[anywhere, vmem],
        out_specs=anywhere,
        scratch_shapes=[
            pltpu.VMEM((most, rows, width), jnp.float32),
            pltpu.VMEM((most, width, rows), jnp.bfloat16),
            dma((most,)),
            dma((peers,)),
            dma((peers,)),
        ],
        compiler_params=pltpu.CompilerParams(
            collective_id=1,
            has_side_effects=True,
            vmem_limit_bytes=6 * most * rows * width + VMEM_FOR_REST,
        ),
    )(in_hbm(master_up), scales)
    up = pl.pallas_call(
        last_land,
        out_shape=local[1],
        in_specs=[hbm, anywhere],
        out_specs=hbm,
        scratch_shapes=[dma],
        input_output_aliases={0: 0},
        compiler_params=small,
    )(up, last)
    return gate.transpose(0, 2, 1), up.transpose(0, 2, 1), scale_gate, scale_up, router.T


def plain(master_gate, master_up, router_weight, router_gain):
    scale_gate, scale_up = lax.pmax(
        (jnp.max(jnp.abs(master_gate), axis=1), jnp.max(jnp.abs(master_up), axis=1)), "rows"
    )
    narrow_gate, narrow_up = (
        (master_gate / jnp.expand_dims(scale_gate, 1)).astype(jnp.bfloat16),
        (master_up / jnp.expand_dims(scale_up, 1)).astype(jnp.bfloat16),
    )
    final_gate, final_up = (
        lax.all_to_all(narrow_gate, "rows", split_axis=2, concat_axis=1, tiled=True),
        lax.all_to_all(narrow_up, "rows", split_axis=2, concat_axis=1, tiled=True),
    )
    scale_gate = lax.dynamic_slice_in_dim(
        scale_gate, lax.axis_index("rows") * final_gate.shape[2], final_gate.shape[2], axis=1
    )
    scale_up = lax.dynamic_slice_in_dim(
        scale_up, lax.axis_index("rows") * final_up.shape[2], final_up.shape[2], axis=1
    )
    part_router = (router_weight * router_gain[:, None]).astype(jnp.bfloat16)
    row_router = lax.all_gather(part_router, "rows", axis=0, tiled=True)
    serve_router = lax.all_gather(row_router, "owner", axis=1, tiled=True)
    return (final_gate, final_up, scale_gate, scale_up, serve_router)


def solution(mesh):
    owners, peers = mesh.shape["owner"], mesh.shape["rows"]

    def shards(master_gate, master_up, router_weight, router_gain):
        experts, rows, width = master_gate.shape
        whole_tiles = (
            peers & (peers - 1) == 0
            and peers > 2
            and rows % LANES == 0
            and width % LANES == 0
            and width % (peers * PACKED) == 0
            and experts % SUBLANES == 0
            and router_weight.shape[1] % PACKED == 0
            and (4 * experts + 4 * SLOTS) * rows * width <= VMEM_FOR_BLOCKS
        )
        run = functools.partial(fused, owners, peers) if whole_tiles else plain
        return run(master_gate, master_up, router_weight, router_gain)

    return jax.shard_map(
        shards,
        mesh=mesh,
        in_specs=(
            P("owner", "rows", None),
            P("owner", "rows", None),
            P("rows", "owner"),
            P("rows"),
        ),
        out_specs=(
            P("owner", None, "rows"),
            P("owner", None, "rows"),
            P("owner", "rows"),
            P("owner", "rows"),
            P(),
        ),
        check_vma=False,
    )
```

```python
import functools

import jax
import jax.numpy as jnp
from jax import lax
from jax.experimental import pallas as pl
from jax.experimental.pallas import tpu as pltpu
from jax.sharding import PartitionSpec as P

MESH = pl.DeviceIdType.MESH
LANES = 128
SUBLANES = 8
PACKED = 16
SLOTS = 5
DIRECT = 2
LATER = (0, 3)
LANDINGS = 4
VMEM_FOR_BLOCKS = 48 * 1024 * 1024
VMEM_FOR_REST = 2 * 1024 * 1024


def half(lower, tiles, far):
    count = -(-tiles // 2)
    if far:
        return jnp.where(lower, tiles - count, 0), count
    return jnp.where(lower, 0, count), tiles - count


def far_targets(me, peers):
    near = peers // 2
    base = near - near * (me // near)
    return [base + p for p in range(near)]


def kernel(
    owners,
    peers,
    gate,
    up,
    router_hbm,
    gain_hbm,
    out_gate,
    out_up,
    out_router,
    out_scale_gate,
    out_scale_up,
    scales_rest,
    slots,
    seen,
    opening,
    largest_first,
    largest_rest,
    scales_first,
    parts_first,
    parts_rest,
    partial_first,
    partial_rest,
    across_first,
    across_rest,
    send,
    router,
    gain,
    row,
    slot_sem,
    small_sem,
    send_sem,
    recv_sem,
    seen_send,
    seen_recv,
    part_send,
    part_recv,
    across_send,
    across_recv,
    whole_send,
    whole_recv,
    router_send,
    router_recv,
):
    owner, me = lax.axis_index("owner"), lax.axis_index("rows")
    experts, rows, width = gate.shape
    tiles = width // LANES
    cut = width // peers
    near = peers // 2
    spot = lax.rem(me, near)
    masters, outs = (gate, up), (out_gate, out_up)
    largest, parts = (largest_first, largest_rest), (parts_first, parts_rest)
    partial, across = (partial_first, partial_rest), (across_first, across_rest)
    scales = (scales_first, scales_rest)
    lanes = pl.ds(pl.multiple_of(me * rows, LANES), rows)

    def partner(k):
        bits = [1 << b for b in range(peers.bit_length() - 1) if k >> b & 1]
        return sum((bit - 2 * bit * lax.rem(me // bit, 2) for bit in bits), me)

    def remote(src, dst, sent, received, to):
        return pltpu.make_async_remote_copy(
            src_ref=src,
            dst_ref=dst,
            send_sem=sent,
            recv_sem=received,
            device_id=to,
            device_id_type=MESH,
        )

    stream = [(0, 0, SUBLANES), (0, 0, DIRECT)]
    if experts > SUBLANES:
        stream.append((0, SUBLANES, experts - SUBLANES))
    stream += [(1, 0, experts), (0, DIRECT, experts - DIRECT)]
    stream.append((1, 0, experts - max(LATER)))
    bases = [sum(length for _, _, length in stream[:q]) for q in range(len(stream))]
    total = sum(length for _, _, length in stream)

    def fetch(m, e, i):
        s = lax.rem(i, SLOTS)
        return pltpu.make_async_copy(masters[m].at[e], slots.at[s], slot_sem.at[s])

    def fetch_start(i):
        for (m, first, length), base in zip(stream, bases):
            if isinstance(i, int):
                if base <= i < base + length:
                    fetch(m, first + i - base, i).start()
            else:

                @pl.when(jnp.logical_and(i >= base, i < base + length))
                def _():
                    fetch(m, first + i - base, i).start()

    def arrived(q, i):
        m, first, _ = stream[q]
        fetch(m, first + i, bases[q] + i).wait()
        return first + i, lax.rem(bases[q] + i, SLOTS)

    def following(q, i, steps):
        ahead = bases[q] + i + SLOTS
        low = bases[q] + SLOTS
        for (m, first, length), base in zip(stream, bases):
            if base + length <= low or base >= low + steps:
                continue
            if base <= low and base + length >= low + steps:
                fetch(m, first + ahead - base, ahead).start()
            else:

                @pl.when(jnp.logical_and(ahead >= base, ahead < base + length))
                def _():
                    fetch(m, first + ahead - base, ahead).start()

    def spots(m, e, c, first):
        k = m * experts + e - (0 if first else SUBLANES)
        return (k // SUBLANES) * tiles + c, pl.ds(k % SUBLANES if isinstance(k, int) else lax.rem(k, SUBLANES), 1)

    def measure(m, e, s, first):
        found = []
        for c in range(tiles):
            x = slots[s, :, c * LANES : (c + 1) * LANES]
            tile, sub = spots(m, e, c, first)
            found.append(jnp.max(jnp.abs(x), axis=0, keepdims=True))
            largest[0 if first else 1][tile, sub, :] = found[-1]
        return found

    def maxima(q, start, first):
        m, _, length = stream[q]

        def body(i, _):
            e, s = arrived(q, i)
            measure(m, e, s, first)
            following(q, i, length)
            return 0

        lax.fori_loop(start, length, body, 0)

    def seen_copy(e, k):
        return remote(
            seen.at[e, 0, pl.ds(0, tiles)],
            seen.at[e, k, pl.ds(0, tiles)],
            seen_send.at[e, k],
            seen_recv.at[e, k],
            {"rows": partner(k)},
        )

    def part_copy(stage, k):
        per = parts[stage].shape[1]
        to = partner(k)
        return remote(
            largest[stage].at[pl.ds(lax.rem(to, near) * per, per)],
            parts[stage].at[k],
            part_send.at[stage, k],
            part_recv.at[stage, k],
            {"rows": to},
        )

    def across_copy(stage):
        return remote(
            partial[stage],
            across[stage],
            across_send.at[stage],
            across_recv.at[stage],
            {"rows": partner(near)},
        )

    def share(stage, of):
        per = parts[stage].shape[1]
        return scales[stage].at[pl.ds(of * per, per)]

    def whole_copy(stage, k):
        return remote(
            share(stage, spot),
            share(stage, spot),
            whole_send.at[stage, k],
            whole_recv.at[stage, k],
            {"rows": partner(k)},
        )

    def scatter(stage):
        for k in range(1, near):
            part_copy(stage, k).start()

    def reduce(stage):
        per = parts[stage].shape[1]
        most = largest[stage][pl.ds(spot * per, per)]
        for k in range(1, near):
            part_copy(stage, k).wait_recv()
            most = jnp.maximum(most, parts[stage][k])
        partial[stage][...] = most
        across_copy(stage).start()

    def spread(stage):
        across_copy(stage).wait_recv()
        share(stage, spot)[...] = jnp.maximum(partial[stage][...], across[stage][...])
        for k in range(1, near):
            whole_copy(stage, k).start()

    def gathered(stage):
        across_copy(stage).wait_send()
        for k in range(1, near):
            part_copy(stage, k).wait_send()
            there = share(stage, lax.rem(partner(k), near))
            pltpu.make_async_copy(there, there, whole_recv.at[stage, k]).wait()
            whole_copy(stage, k).wait_send()

    def send_copy(m, to, e, length):
        return remote(
            send.at[m, pl.ds(e, length), pl.ds(pl.multiple_of(to * cut, PACKED), cut), :],
            outs[m].at[pl.ds(e, length), :, lanes],
            send_sem.at[m, to],
            recv_sem.at[m, me],
            {"rows": to},
        )

    def sent_and_received(m, length):
        for to in [partner(k) for k in range(1, peers)]:
            send_copy(m, to, 0, length).wait_send()
            there = outs[m].at[pl.ds(0, length), :, pl.ds(pl.multiple_of(to * rows, LANES), rows)]
            pltpu.make_async_copy(there, there, recv_sem.at[m, to]).wait()

    def keep_copy(m, e, length):
        return pltpu.make_async_copy(
            send.at[m, pl.ds(e, length), pl.ds(pl.multiple_of(me * cut, PACKED), cut), :],
            outs[m].at[pl.ds(e, length), :, lanes],
            send_sem.at[m, me],
        )

    across_from = far_targets(me, peers)
    held = across_from[near // 2 :]

    def rescale(m, e, s, scale_of, low, count):
        for c in range(count):
            at = pl.ds(pl.multiple_of((low + c) * LANES, LANES), LANES)
            send[m, e, at, :] = (slots[s, :, at] / scale_of(low + c)).T.astype(send.dtype)

    def send_near(m, e):
        for k in range(1, near):
            send_copy(m, partner(k), e, 1).start()
        keep_copy(m, e, 1).start()

    def one(m, e, s, scale_of):
        rescale(m, e, s, scale_of, 0, tiles)
        send_near(m, e)
        for to in across_from:
            send_copy(m, to, e, 1).start()

    def bulk(q, start, stop, first):
        m, _, _ = stream[q]

        def body(i, _):
            e, s = arrived(q, i)

            def scale_of(c):
                tile, sub = spots(m, e, c, first)
                return scales[0 if first else 1][tile, sub, :]

            one(m, e, s, scale_of)
            following(q, i, stream[q][2])
            return 0

        lax.fori_loop(start, stop, body, 0)

    def early(q, i, hold):
        e = stream[q][1] + i
        for k in range(1, peers):
            seen_copy(e, k).wait_recv()
        opening[e, :tiles, :] = jnp.max(seen[e, :, :tiles, :], axis=0)
        _, s = arrived(q, i)

        def scale_of(c):
            return opening[e, pl.ds(c, 1), :]

        rescale(0, e, s, scale_of, *half(me < near, tiles, True))
        for to in across_from[: near // 2] if hold else across_from:
            send_copy(0, to, e, 1).start()
        rescale(0, e, s, scale_of, *half(me < near, tiles, False))
        send_near(0, e)
        fetch_start(bases[q] + i + SLOTS)

    depth = router.shape[0]
    mine = pl.ds(pl.multiple_of(owner * depth, PACKED), depth)

    def block(of):
        return out_router.at[mine, pl.ds(pl.multiple_of(of * rows, LANES), rows)]

    def router_across():
        return remote(row, block(me), router_send.at[0], router_recv.at[0], {"rows": partner(near)})

    def router_near(k, far):
        of = partner(near) if far else me
        return remote(
            block(of) if far else row,
            block(of),
            router_send.at[1 + 2 * k + far],
            router_recv.at[1 + 2 * k + far],
            {"rows": partner(k)},
        )

    def router_near_arrival(k, far):
        there = block(partner(near + k) if far else partner(k))
        return pltpu.make_async_copy(there, there, router_recv.at[1 + 2 * k + far])

    def router_owner(j):
        return remote(
            out_router.at[mine],
            out_router.at[mine],
            router_send.at[peers + j],
            router_recv.at[peers + j],
            {"owner": lax.rem(owner + j, owners)},
        )

    def router_owner_arrival(j):
        from_owner = lax.rem(owner + owners - j, owners)
        there = out_router.at[pl.ds(pl.multiple_of(from_owner * depth, PACKED), depth)]
        return pltpu.make_async_copy(there, there, router_recv.at[peers + j])

    barrier = pltpu.get_barrier_semaphore()

    fetch_start(0)
    for k in range(1, peers):
        pl.semaphore_signal(barrier, inc=1, device_id={"rows": partner(k)}, device_id_type=MESH)
    for j in range(1, owners):
        pl.semaphore_signal(
            barrier,
            inc=1,
            device_id={"owner": lax.rem(owner + j, owners)},
            device_id_type=MESH,
        )
    smalls = [
        pltpu.make_async_copy(router_hbm, router, small_sem.at[0]),
        pltpu.make_async_copy(gain_hbm, gain, small_sem.at[1]),
    ]
    largest_first[...] = jnp.zeros_like(largest_first)
    largest_rest[...] = jnp.zeros_like(largest_rest)
    for e in range(DIRECT):
        _, s = arrived(0, e)
        if e == 0:
            for i in range(1, SLOTS):
                fetch_start(i)
        found = measure(0, e, s, True)
        for c in range(tiles):
            seen[e, 0, c : c + 1, :] = found[c]
        if e == 0:
            for copy in smalls:
                copy.start()
            pl.semaphore_wait(barrier, peers - 1 + owners - 1)
        for k in range(1, peers):
            seen_copy(e, k).start()
        fetch_start(e + SLOTS)
    for copy in smalls:
        copy.wait()
    row[...] = (router[...] * gain[...]).astype(row.dtype)
    router_across().start()
    keep_router = pltpu.make_async_copy(row, block(me), small_sem.at[0])
    keep_router.start()
    maxima(0, DIRECT, True)
    scatter(0)
    early(1, 0, False)
    reduce(0)
    early(1, 1, True)
    rest = 2
    if experts > SUBLANES:
        maxima(rest, 0, False)
        rest += 1
    maxima(rest, 0, False)
    rest += 1
    router_across().wait_recv()
    for k in range(1, near):
        router_near(k, 0).start()
        router_near(k, 1).start()
    spread(0)
    scatter(1)
    for to in held:
        send_copy(0, to, 1, 1).start()
    gathered(0)
    bulk(rest, 0, 1, True)
    reduce(1)
    bulk(rest, 1, 2, True)
    spread(1)
    bulk(rest, 2, SUBLANES - DIRECT, True)
    gathered(1)
    if experts > SUBLANES:
        bulk(rest, SUBLANES - DIRECT, experts - DIRECT, False)
    keep_router.wait()
    router_across().wait_send()
    for k in range(1, near):
        for far in range(2):
            router_near_arrival(k, far).wait()
            router_near(k, far).wait_send()
    for j in range(1, owners):
        router_owner(j).start()
    bulk(rest + 1, 0, experts - max(LATER), False)
    for turn, later in enumerate(LATER):
        if later == max(LATER):
            continue

        @pl.when(lax.rem(owner, len(LATER)) == turn)
        def _():
            extra = max(LATER) - later
            low = experts - max(LATER)
            for i in range(extra):
                fetch(1, low + i, i).start()

            def body(i, _):
                fetch(1, low + i, i).wait()

                def scale_of(c):
                    tile, sub = spots(1, low + i, c, False)
                    return scales_rest[tile, sub, :]

                one(1, low + i, i, scale_of)
                return 0

            lax.fori_loop(0, extra, body, 0)


    for at in range(peers):

        @pl.when(me == at)
        def _():
            low = at * cut // LANES
            high = -(-(at + 1) * cut // LANES)
            for m in range(2):
                for e in range(0, experts, SUBLANES):
                    first = m == 0 and e == 0
                    found = []
                    for c in range(low, high):
                        k = m * experts + e - (0 if first else SUBLANES)
                        found.append(scales[0 if first else 1][(k // SUBLANES) * tiles + c])
                    found = jnp.concatenate(found, axis=1)
                    begin = at * cut - low * LANES
                    out = (out_scale_gate, out_scale_up)[m]
                    out[e : e + SUBLANES, :] = found[:, begin : begin + cut]

    for e in range(DIRECT):
        for k in range(1, peers):
            seen_copy(e, k).wait_send()
    for j in range(1, owners):
        router_owner_arrival(j).wait()
        router_owner(j).wait_send()
    keep_copy(0, 0, experts).wait()
    sent_and_received(0, experts)
    for turn, later in enumerate(LATER):

        @pl.when(lax.rem(owner, len(LATER)) == turn)
        def _():
            keep_copy(1, 0, experts - later).wait()
            sent_and_received(1, experts - later)


def last_kernel(peers, up, scales, out, slots, send, slot_sem, send_sem, recv_sem):
    owner, me = lax.axis_index("owner"), lax.axis_index("rows")
    experts, rows, width = up.shape
    tiles = width // LANES
    cut = width // peers
    lanes = pl.ds(pl.multiple_of(me * rows, LANES), rows)
    near = peers // 2
    turn = lax.rem(owner, len(LATER))
    later = sum(jnp.where(turn == t, n, 0) for t, n in enumerate(LATER))

    def partner(k):
        bits = [1 << b for b in range(peers.bit_length() - 1) if k >> b & 1]
        return sum((bit - 2 * bit * lax.rem(me // bit, 2) for bit in bits), me)

    def fetch(i):
        return pltpu.make_async_copy(
            up.at[experts - later + i], slots.at[i], slot_sem.at[i]
        )

    def prepare(i):
        fetch(i).wait()
        sub = pl.ds(SUBLANES - later + i, 1)
        for c in range(tiles):
            x = slots[i, :, c * LANES : (c + 1) * LANES]
            send[i, c * LANES : (c + 1) * LANES, :] = (x / scales[c, sub, :]).T.astype(send.dtype)

    def send_copy(to, i, length):
        return pltpu.make_async_remote_copy(
            src_ref=send.at[pl.ds(i, length), pl.ds(pl.multiple_of(to * cut, PACKED), cut), :],
            dst_ref=out.at[pl.ds(i, length), :, lanes],
            send_sem=send_sem.at[to],
            recv_sem=recv_sem.at[me],
            device_id={"rows": to},
            device_id_type=MESH,
        )

    def keep_copy(i, length):
        return pltpu.make_async_copy(
            send.at[pl.ds(i, length), pl.ds(pl.multiple_of(me * cut, PACKED), cut), :],
            out.at[pl.ds(i, length), :, lanes],
            send_sem.at[me],
        )

    def post(i):
        for k in range(1, near):
            send_copy(partner(k), i, 1).start()
        for to in far_targets(me, peers):
            send_copy(to, i, 1).start()
        keep_copy(i, 1).start()

    barrier = pltpu.get_barrier_semaphore()
    for k in range(1, peers):
        pl.semaphore_signal(barrier, inc=1, device_id={"rows": partner(k)}, device_id_type=MESH)

    def begin(i, _):
        fetch(i).start()
        return 0

    lax.fori_loop(0, later, begin, 0)
    if min(LATER) > 0:
        prepare(0)
    else:
        pl.when(later > 0)(lambda: prepare(0))
    pl.semaphore_wait(barrier, peers - 1)
    if min(LATER) > 0:
        post(0)
    else:
        pl.when(later > 0)(lambda: post(0))

    def body(i, _):
        prepare(i)
        post(i)
        return 0

    lax.fori_loop(1, later, body, 0)
    for t, n in enumerate(LATER):
        if n == 0:
            continue

        @pl.when(turn == t)
        def _():
            keep_copy(0, n).wait()
            for to in [partner(k) for k in range(1, peers)]:
                send_copy(to, 0, n).wait_send()
                there = out.at[pl.ds(0, n), :, pl.ds(pl.multiple_of(to * rows, LANES), rows)]
                pltpu.make_async_copy(there, there, recv_sem.at[to]).wait()


def land(gate, up, router, scale_gate, scale_up, scales, *refs):
    outs, last_scales, sem = refs[:5], refs[5], refs[6]
    tiles = last_scales.shape[0]
    experts = gate.shape[0]

    def move(i, a, b, low, high, pieces):
        cuts = [low + (high - low) * j // pieces for j in range(pieces + 1)]
        for at, end in zip(cuts, cuts[1:]):
            span = pl.ds(at, end - at)
            pltpu.make_async_copy(a.at[span], b.at[span], sem.at[i]).start()

    def moved(i, a, b, low, high):
        span = pl.ds(low, high - low)
        pltpu.make_async_copy(a.at[span], b.at[span], sem.at[i]).wait()

    whole = [(0, gate), (2, router), (3, scale_gate), (4, scale_up)]
    for i, a in whole:
        move(i, a, outs[i], 0, a.shape[0], LANDINGS if i == 0 else 1)
    for turn, later in enumerate(LATER):

        @pl.when(lax.rem(lax.axis_index("owner"), len(LATER)) == turn)
        def _():
            move(1, up, outs[1], 0, experts - later, LANDINGS)
            moved(1, up, outs[1], 0, experts - later)

    low = (2 * experts // SUBLANES - 2) * tiles
    last_scales[...] = scales[low : low + tiles]
    for i, a in whole:
        moved(i, a, outs[i], 0, a.shape[0])


def last_land(_, last, up, sem):
    experts = up.shape[0]
    for turn, later in enumerate(LATER):
        if later == 0:
            continue

        @pl.when(lax.rem(lax.axis_index("owner"), len(LATER)) == turn)
        def _():
            for i in range(later):
                there = up.at[pl.ds(experts - later + i, 1)]
                pltpu.make_async_copy(last.at[pl.ds(i, 1)], there, sem).start()
            there = up.at[pl.ds(experts - later, later)]
            pltpu.make_async_copy(last.at[pl.ds(0, later)], there, sem).wait()


def fused(owners, peers, master_gate, master_up, router_weight, router_gain):
    experts, rows, width = master_gate.shape
    cut = width // peers
    near = peers // 2
    tiles = width // LANES
    padded = -(-tiles // SUBLANES) * SUBLANES
    groups = 2 * experts // SUBLANES
    first, rest = -(-tiles // near), -(-(groups - 1) * tiles // near)
    depth = router_weight.shape[1]
    anywhere = pl.BlockSpec(memory_space=pl.ANY)
    vmem = pl.BlockSpec(memory_space=pltpu.VMEM)
    hbm = pl.BlockSpec(memory_space=pltpu.HBM)
    dma = pltpu.SemaphoreType.DMA
    turned = jax.ShapeDtypeStruct((experts, cut, rows * peers), jnp.bfloat16)
    scale = jax.ShapeDtypeStruct((experts, cut), jnp.float32)

    def in_hbm(a):
        return pltpu.with_memory_space_constraint(a, pltpu.HBM)

    def maxima(*shape):
        return pltpu.VMEM((*shape, SUBLANES, LANES), jnp.float32)

    landed = pl.pallas_call(
        functools.partial(kernel, owners, peers),
        out_shape=(
            turned,
            turned,
            jax.ShapeDtypeStruct((depth * owners, rows * peers), jnp.bfloat16),
            scale,
            scale,
            jax.ShapeDtypeStruct((rest * near, SUBLANES, LANES), jnp.float32),
        ),
        in_specs=[anywhere, anywhere, hbm, hbm],
        out_specs=(anywhere, anywhere, anywhere, vmem, vmem, vmem),
        scratch_shapes=[
            pltpu.VMEM((SLOTS, rows, width), jnp.float32),
            pltpu.VMEM((DIRECT, peers, padded, LANES), jnp.float32),
            pltpu.VMEM((DIRECT, padded, LANES), jnp.float32),
            maxima(first * near),
            maxima(rest * near),
            maxima(first * near),
            maxima(near, first),
            maxima(near, rest),
            maxima(first),
            maxima(rest),
            maxima(first),
            maxima(rest),
            pltpu.VMEM((2, experts, width, rows), jnp.bfloat16),
            pltpu.VMEM((depth, rows), jnp.float32),
            pltpu.VMEM((1, rows), jnp.float32),
            pltpu.VMEM((depth, rows), jnp.bfloat16),
            dma((SLOTS,)),
            dma((2,)),
            dma((2, peers)),
            dma((2, peers)),
            dma((DIRECT, peers)),
            dma((DIRECT, peers)),
            dma((2, near)),
            dma((2, near)),
            dma((2,)),
            dma((2,)),
            dma((2, near)),
            dma((2, near)),
            dma((peers + owners,)),
            dma((peers + owners,)),
        ],
        compiler_params=pltpu.CompilerParams(
            collective_id=0,
            has_side_effects=True,
            vmem_limit_bytes=(4 * experts + 4 * SLOTS) * rows * width + VMEM_FOR_REST,
        ),
    )(*(in_hbm(a) for a in (master_gate, master_up, router_weight.T, router_gain[None, :])))
    local = [jax.ShapeDtypeStruct(a.shape, a.dtype) for a in landed[:5]]
    small = pltpu.CompilerParams(vmem_limit_bytes=VMEM_FOR_REST)
    gate, up, router, scale_gate, scale_up, scales = pl.pallas_call(
        land,
        out_shape=[*local, jax.ShapeDtypeStruct((tiles, SUBLANES, LANES), jnp.float32)],
        in_specs=[anywhere] * 5 + [vmem],
        out_specs=[hbm] * 5 + [vmem],
        scratch_shapes=[dma((5,))],
        compiler_params=small,
    )(*landed)
    most = max(LATER)
    last = pl.pallas_call(
        functools.partial(last_kernel, peers),
        out_shape=jax.ShapeDtypeStruct((most, cut, rows * peers), jnp.bfloat16),
        in_specs=[anywhere, vmem],
        out_specs=anywhere,
        scratch_shapes=[
            pltpu.VMEM((most, rows, width), jnp.float32),
            pltpu.VMEM((most, width, rows), jnp.bfloat16),
            dma((most,)),
            dma((peers,)),
            dma((peers,)),
        ],
        compiler_params=pltpu.CompilerParams(
            collective_id=1,
            has_side_effects=True,
            vmem_limit_bytes=6 * most * rows * width + VMEM_FOR_REST,
        ),
    )(in_hbm(master_up), scales)
    up = pl.pallas_call(
        last_land,
        out_shape=local[1],
        in_specs=[hbm, anywhere],
        out_specs=hbm,
        scratch_shapes=[dma],
        input_output_aliases={0: 0},
        compiler_params=small,
    )(up, last)
    return gate.transpose(0, 2, 1), up.transpose(0, 2, 1), scale_gate, scale_up, router.T


def plain(master_gate, master_up, router_weight, router_gain):
    scale_gate, scale_up = lax.pmax(
        (jnp.max(jnp.abs(master_gate), axis=1), jnp.max(jnp.abs(master_up), axis=1)), "rows"
    )
    narrow_gate, narrow_up = (
        (master_gate / jnp.expand_dims(scale_gate, 1)).astype(jnp.bfloat16),
        (master_up / jnp.expand_dims(scale_up, 1)).astype(jnp.bfloat16),
    )
    final_gate, final_up = (
        lax.all_to_all(narrow_gate, "rows", split_axis=2, concat_axis=1, tiled=True),
        lax.all_to_all(narrow_up, "rows", split_axis=2, concat_axis=1, tiled=True),
    )
    scale_gate = lax.dynamic_slice_in_dim(
        scale_gate, lax.axis_index("rows") * final_gate.shape[2], final_gate.shape[2], axis=1
    )
    scale_up = lax.dynamic_slice_in_dim(
        scale_up, lax.axis_index("rows") * final_up.shape[2], final_up.shape[2], axis=1
    )
    part_router = (router_weight * router_gain[:, None]).astype(jnp.bfloat16)
    row_router = lax.all_gather(part_router, "rows", axis=0, tiled=True)
    serve_router = lax.all_gather(row_router, "owner", axis=1, tiled=True)
    return (final_gate, final_up, scale_gate, scale_up, serve_router)


def solution(mesh):
    owners, peers = mesh.shape["owner"], mesh.shape["rows"]

    def shards(master_gate, master_up, router_weight, router_gain):
        experts, rows, width = master_gate.shape
        whole_tiles = (
            peers & (peers - 1) == 0
            and peers > 2
            and rows % LANES == 0
            and width % LANES == 0
            and width % (peers * PACKED) == 0
            and experts % SUBLANES == 0
            and router_weight.shape[1] % PACKED == 0
            and (4 * experts + 4 * SLOTS) * rows * width <= VMEM_FOR_BLOCKS
        )
        run = functools.partial(fused, owners, peers) if whole_tiles else plain
        return run(master_gate, master_up, router_weight, router_gain)

    return jax.shard_map(
        shards,
        mesh=mesh,
        in_specs=(
            P("owner", "rows", None),
            P("owner", "rows", None),
            P("rows", "owner"),
            P("rows"),
        ),
        out_specs=(
            P("owner", None, "rows"),
            P("owner", None, "rows"),
            P("owner", "rows"),
            P("owner", "rows"),
            P(),
        ),
        check_vma=False,
    )
```
